128 devices in a mesh: dp: 16 (over z, x), mp: 8 (over y, core).
Axes of the slice: x: 4, y: 4, z: 4, core: 2. Of those that a mesh axis runs over, the one named last changes fastest.
Arguments:
- patches: bfloat16 [24576, 1280], P('dp', 'mp'), may hold values from -6 to 6
- cotangent: bfloat16 [24576, 1280], P('dp', 'mp'), may hold values from -0.29882812 to 0.29882812
- encoder_rank: int32 [192], P('dp'), may hold values from 0 to 15, as said below
- block_fill: int32 [192], P('dp'), may hold values from 32 to 128
- w_up: bfloat16 [1280, 5120], P(None, 'mp'), may hold values from -0.15625 to 0.15625
- w_down: bfloat16 [5120, 1280], P('mp'), may hold values from -0.078125 to 0.078125
- q_up: float32 [5120, 64], P('mp'), may hold values from -6 to 6
- q_down: float32 [1280, 64], replicated, may hold values from -6 to 6
Outputs:
- encoded: bfloat16 [36864, 1280], P('dp', 'mp')
- approx_up: float32 [1280, 5120], P(None, 'mp')
- approx_down: float32 [5120, 1280], P('mp')
- qnew_up: float32 [5120, 64], P('mp')
- qnew_down: float32 [1280, 64], replicated
The draws below stay inside these ranges and needn't reach their ends.
Inputs may be any that keep to these rules, and one draw needn't show every extreme that they name: `encoder_rank`: from the blocks of one data rank at most 2 go to one encoder rank, and one encoder rank receives at most 18 blocks in all; both bounds are reached in every draw. Every encoder rank receives some block.
All inputs are finite; a program needn't handle non-finite values.
Results may differ from the reference program's by a relative error of at most 0.015.
Values may be sent and summed in bfloat16 or wider, within the bound.
A program may use at most 128 MiB of HBM per device.

```python
import jax
import jax.numpy as jnp
from jax import lax

D = 1280
FF = 5120
BLOCK = 128
RANK = 64
BLK_DEV = 12
RMAX = 18
BLOCKS = 192
TOKENS = 24576
N_DP = 16


def draw_encoder_rank(key, part):
    base_key = jax.random.fold_in(key, 7)
    key_order, key_shift, key_column = jax.random.split(base_key, 3)
    ordering = jax.random.permutation(key_order, N_DP).astype(jnp.int32)
    uniform_cols = BLK_DEV - 2
    hot_count = N_DP // 4
    shifts = jax.random.permutation(key_shift, N_DP)[:uniform_cols].astype(jnp.int32)
    sources = jnp.arange(N_DP, dtype=jnp.int32)
    spread = (sources[:, None] + shifts[None, :]) % N_DP
    lead_col = spread[:, 0]
    hot_index = (lead_col[:, None] + jnp.arange(2, dtype=jnp.int32)[None, :]) % hot_count
    dest_table = jnp.concatenate([spread, hot_index], axis=1)
    columns = jax.random.permutation(key_column, BLK_DEV)
    dest_table = dest_table[:, columns]
    return ordering[dest_table].reshape(-1).astype(jnp.int32)


def place_ends(values, own_key, smallest, top_value):
    place = [jax.random.randint(jax.random.fold_in(own_key, axis), (), 0, length) for axis, length in enumerate(values.shape)]
    widest = values.shape.index(max(values.shape))
    next_to = place[:widest] + [(place[widest] + 1) % values.shape[widest]] + place[widest + 1:]
    return values.at[tuple(place)].set(smallest).at[tuple(next_to)].set(top_value)


def levels(own_key, dims, cuts, low, top_value):
    def one(dim, blocks):
        steps = jax.random.uniform(jax.random.fold_in(jax.random.fold_in(own_key, 6), dim), (blocks,), jnp.float32, low / len(cuts), top_value / len(cuts))
        return jnp.repeat(jnp.exp(steps), dims[dim] // blocks).reshape((-1,) + (1,) * (len(dims) - dim - 1))

    loudness = one(*cuts[0])
    for cut in cuts[1:]:
        loudness = loudness * one(*cut)
    return loudness


def gaussian(stream_key, extent, deviation, most, shards=(), held_as=jnp.bfloat16):
    gain = levels(stream_key, extent, shards, -0.22, 0.18) if shards else 1.0
    entries = jax.random.normal(stream_key, extent, jnp.float32) * deviation * gain
    return jnp.minimum(jnp.maximum(entries, -most), most).astype(held_as)


def setup_inputs(seed: int = 0) -> dict:
    keys = jax.random.split(jax.random.key(seed), 9)
    patches = gaussian(keys[0], (TOKENS, D), 1.0, 6.0, ((0, 16), (1, 8)))
    cotangent = gaussian(keys[1], (TOKENS, D), 0.05, 0.29882812, ((0, 16), (1, 8)))
    encoder_rank = draw_encoder_rank(jax.random.fold_in(keys[8], 71), 0)
    block_fill = place_ends(jax.random.randint(keys[3], (BLOCKS,), BLOCK // 4, BLOCK + 1), jax.random.fold_in(keys[3], 1), BLOCK // 4, BLOCK).astype(jnp.int32)
    w_up = gaussian(keys[4], (D, FF), D ** -0.5, 0.15625, ((1, 8),))
    w_down = gaussian(keys[5], (FF, D), FF ** -0.5, 0.078125, ((0, 8),))
    q_up = gaussian(keys[6], (FF, RANK), 1.0, 6.0, ((0, 8),), jnp.float32)
    q_down = gaussian(keys[7], (D, RANK), 1.0, 6.0, (), jnp.float32)
    return dict(patches=patches, cotangent=cotangent, encoder_rank=encoder_rank, block_fill=block_fill, w_up=w_up, w_down=w_down, q_up=q_up, q_down=q_down)


def gelu_parts(preact):
    sig = jax.nn.sigmoid(1.702 * preact)
    return (preact * sig, sig + 1.702 * preact * sig * (1.0 - sig))

def compress(grad, warm):
    highest = lax.Precision.HIGHEST
    proj = jnp.dot(grad, warm, precision=highest)
    gram = jnp.dot(proj.T, proj, precision=highest)
    lower = jnp.linalg.cholesky(gram)
    basis = jax.scipy.linalg.solve_triangular(lower, proj.T, lower=True).T
    fresh = jnp.dot(grad.T, basis, precision=highest)
    return (fresh, jnp.dot(basis, fresh.T, precision=highest))

def reference(patches, cotangent, encoder_rank, block_fill, w_up, w_down, q_up, q_down):
    total_rows = patches.shape[0]
    row_ids = jnp.arange(total_rows, dtype=jnp.int32)
    within = row_ids % BLOCK
    owner = row_ids // BLOCK
    keep = (within < block_fill[owner])[:, None]
    preact = jnp.dot(patches.astype(jnp.float32), w_up.astype(jnp.float32), preferred_element_type=jnp.float32)
    active, slope = gelu_parts(preact)
    hidden = active.astype(jnp.bfloat16)
    out_rows = jnp.where(keep, jnp.dot(hidden.astype(jnp.float32), w_down.astype(jnp.float32), preferred_element_type=jnp.float32), 0.0).astype(jnp.bfloat16)
    masked_cot = jnp.where(keep, cotangent, jnp.zeros((), jnp.bfloat16))
    grad_hidden = lax.dot_general(masked_cot.astype(jnp.float32), w_down.astype(jnp.float32), (((1,), (1,)), ((), ())), preferred_element_type=jnp.float32)
    grad_pre = (grad_hidden * slope).astype(jnp.bfloat16)
    grad_up = lax.dot_general(patches.astype(jnp.float32), grad_pre.astype(jnp.float32), (((0,), (0,)), ((), ())), preferred_element_type=jnp.float32)
    grad_down = lax.dot_general(hidden.astype(jnp.float32), masked_cot.astype(jnp.float32), (((0,), (0,)), ((), ())), preferred_element_type=jnp.float32)
    block_ids = jnp.arange(BLOCKS, dtype=jnp.int32)
    before = (encoder_rank[None, :] == encoder_rank[:, None]) & (block_ids[None, :] < block_ids[:, None])
    ordinal = jnp.sum(before.astype(jnp.int32), axis=1).astype(jnp.int32)
    target = (encoder_rank * RMAX + ordinal).astype(jnp.int32)
    placed = jnp.zeros((N_DP * RMAX, BLOCK, D), jnp.bfloat16)
    placed = placed.at[target].set(out_rows.reshape(BLOCKS, BLOCK, D))
    encoded = placed.reshape(N_DP * RMAX * BLOCK, D)
    qnew_up, approx_up = compress(grad_up, q_up)
    qnew_down, approx_down = compress(grad_down, q_down)
    return (encoded, approx_up, approx_down, qnew_up, qnew_down)
```

```python
import jax
import jax.numpy as jnp
from jax import lax
from jax.experimental import pallas as pl
from jax.experimental.pallas import tpu as pltpu
from jax.sharding import PartitionSpec as P

BLOCK = 128
CAP = 2
RMAX = 18
N_DP = 16
N_Y = 4
N_MP = 8
RANK = 64
NC = 6
HALF = NC // 2
AHEAD = 2
MESH = pl.DeviceIdType.MESH
F32 = jnp.float32
BF16 = jnp.bfloat16
NT = (((1,), (1,)), ((), ()))
TN = (((0,), (0,)), ((), ()))


def mm(a, b):
    return jnp.dot(a, b, preferred_element_type=F32)


def mm_nt(a, b):
    return lax.dot_general(a, b, NT, preferred_element_type=F32)


def mm_tn(a, b):
    return lax.dot_general(a, b, TN, preferred_element_type=F32)


def parts(v):
    hi = v.astype(BF16)
    lo = (v - hi.astype(F32)).astype(BF16)
    return hi, lo


def stack2(v):
    return jnp.concatenate(parts(v), axis=0)


def fold2(v):
    return v[:RANK] + v[RANK:]


def left3(v):
    hi, lo = parts(v)
    return jnp.concatenate([hi, hi, lo], axis=0)


def right3(v):
    hi, lo = parts(v)
    return jnp.concatenate([hi, lo, hi], axis=0)


def gram_of(v):
    s = stack2(v)
    g = mm_nt(s, s)
    return g[:RANK, :RANK] + g[:RANK, RANK:] + g[RANK:, :RANK] + g[RANK:, RANK:]


def inverse_factors(grams):
    n = RANK
    row = lax.broadcasted_iota(jnp.int32, (2, n, 2 * n), 1)
    lane = lax.broadcasted_iota(jnp.int32, (2, n, 2 * n), 2)
    eye = jnp.where(lane == row + n, 1.0, 0.0).astype(F32)
    w = jnp.concatenate([grams, jnp.zeros_like(grams)], axis=2) + eye
    for k in range(n - 1):
        pivot = w[:, k : k + 1, k : k + 1]
        line = w[:, k : k + 1, :] * (1.0 / pivot)
        column = w[:, :, k : k + 1]
        w = w - jnp.where(row > k, column * line, 0.0)
    diag = jnp.sum(jnp.where(lane == row, w, 0.0), axis=2, keepdims=True)
    return (w * lax.rsqrt(diag))[:, :, n:]


def kernel_body(
    slot_idx, xin, cin, wu, wd, qu, qd, er, keep,
    a2o, era_out, a3u, b3u, a3d, b3d, qnu, qnd,
    xall, call, hid, gp, wut, wdt, quh, qdh,
    proj, small, pbuf, rsb, rcv, ysend, ybuf, agb, bigf,
    gbuf, outp, po, osb, ra, rb, da, db, fa, fb, ea, eb, ob, a2s, a2r, erb,
    gs, gr, os_, or_, ys, yr, ars, arr, gms, gmr, ers, err_, a2ss, a2rr,
):
    dp = lax.axis_index("dp")
    mp = lax.axis_index("mp")
    y = mp // 2
    c = mp % 2
    right = ((y + 1) % N_Y) * 2 + c
    left = ((y + 3) % N_Y) * 2 + c
    far = ((y + 2) % N_Y) * 2 + c
    mate = y * 2 + (1 - c)
    feats = xin.shape[1]
    tc = xin.shape[2]
    half = proj.shape[3]

    def send(src, dst, ssem, rsem, dpi, mpi):
        return pltpu.make_async_remote_copy(
            src_ref=src, dst_ref=dst, send_sem=ssem, recv_sem=rsem,
            device_id=(dpi, mpi), device_id_type=MESH,
        )

    def dp_at(t):
        return (dp + t) % N_DP

    def mp_at(t):
        return (mp + t) % N_MP

    barrier = pltpu.get_barrier_semaphore()
    for t in range(1, N_DP):
        pl.semaphore_signal(barrier, inc=1, device_id=(dp_at(t), mp), device_id_type=MESH)
    for t in range(1, N_MP):
        pl.semaphore_signal(barrier, inc=1, device_id=(dp, mp_at(t)), device_id_type=MESH)
    pl.semaphore_wait(barrier, N_DP + N_MP - 2)

    def rows(ref, i, owner):
        return ref.at[i, pl.ds(pl.multiple_of(owner * feats, 32), feats), :]

    def own_copy(i, slot):
        src, all_, to = {
            0: (xin, xall, right), 1: (cin, call, left), 2: (cin, call, right),
            3: (xin, xall, left), 6: (xin, xall, mate), 7: (cin, call, mate),
        }[slot]
        return send(src.at[i], rows(all_, i, mp), gs.at[i, slot], gr.at[i, slot], dp, to)

    def pass_copy(i, slot):
        all_, owner, to = {
            4: (xall, left, right), 5: (call, right, left),
            8: (xall, left, mate), 9: (call, right, mate), 10: (call, left, mate),
            11: (xall, right, mate), 12: (xall, far, mate), 13: (call, far, mate),
        }[slot]
        return send(rows(all_, i, owner), rows(all_, i, owner), gs.at[i, slot], gr.at[i, slot], dp, to)

    def start_own(i):
        for slot in (0, 1, 2, 3):
            own_copy(i, slot).start()

    def start_mate(i):
        for slot in (6, 7):
            own_copy(i, slot).start()

    def got(i, slot):
        (own_copy if slot in (0, 1, 2, 3, 6, 7) else pass_copy)(i, slot).wait_recv()

    for i in range(AHEAD):
        start_own(i)
    for i in range(NC):
        start_mate(i)
    for t in range(1, N_DP):
        send(er, erb.at[dp], ers.at[t], err_.at[t], dp_at(t), mp).start()

    erb[dp] = er[...]
    for i in range(NC):
        xall[i, pl.ds(pl.multiple_of(mp * feats, 32), feats), :] = xin[i]
        call[i, pl.ds(pl.multiple_of(mp * feats, 32), feats), :] = cin[i]
    ff = wu.shape[1]
    for j in range(ff // 128):
        wut[j * 128 : (j + 1) * 128, :] = wu[:, j * 128 : (j + 1) * 128].T
    for j in range(wd.shape[1] // 128):
        wdt[j * 128 : (j + 1) * 128, :] = wd[:, j * 128 : (j + 1) * 128].T
    quh[...] = stack2(qu[...])
    qdh[...] = stack2(qd[...])
    proj[0] = jnp.zeros_like(proj[0])
    small[0] = jnp.zeros_like(small[0])
    proj[1] = jnp.zeros_like(proj[1])
    small[1] = jnp.zeros_like(small[1])

    def out_copy(i):
        return send(outp.at[i, 1 - c], po.at[i], os_.at[i], or_.at[i], dp, mate)

    def out_sum(i):
        out_copy(i).wait_recv()
        osb[i] = (outp[i, c].astype(F32) + po[i].astype(F32)).astype(BF16)

    def work_a(i):
        pre = mm(wut[...], xall[i])
        grad = mm(wd[...], call[i])
        sig = jax.nn.sigmoid(1.702 * pre)
        act = pre * sig
        hid[i] = act.astype(BF16)
        gp[i] = (grad * (sig + 1.702 * act * (1.0 - sig))).astype(BF16)

    def work_b(i):
        o = mm(wdt[...], hid[i]).astype(BF16)
        for m in range(N_MP):
            at = (m // 2) * feats
            outp[i, m % 2, at : at + feats, :] = o[m * feats : (m + 1) * feats]
        out_copy(i).start()

    def add_projection(ph, i, left_u, left_d):
        if ph == 0:
            t = fold2(mm(left_u, gp[i]))
            u = fold2(mm(left_d, call[i]))
            big_rhs, small_rhs = xall[i], hid[i]
        else:
            u = fold2(mm(left_u, xall[i]))
            t = fold2(mm(left_d, hid[i]))
            big_rhs, small_rhs = call[i], gp[i]
        big = fold2(mm_nt(stack2(t), big_rhs))
        proj[ph, 0] += big[:, :half]
        proj[ph, 1] += big[:, half:]
        small[ph] += fold2(mm_nt(stack2(u), small_rhs))

    def step(i, carry):
        @pl.when(i < NC)
        def _():
            got(i, 0)
            got(i, 1)
            pass_copy(i, 4).start()
            pass_copy(i, 5).start()
            pass_copy(i, 8).start()
            pass_copy(i, 9).start()

            @pl.when(i + AHEAD < NC)
            def _():
                start_own(i + AHEAD)

        @pl.when(i > 0)
        def _():
            work_a(i - 1)

        @pl.when(i < NC)
        def _():
            got(i, 2)
            got(i, 3)
            pass_copy(i, 10).start()
            pass_copy(i, 11).start()

        @pl.when(i > 0)
        def _():
            add_projection(0, i - 1, quh[...], qdh[...])

        @pl.when(i > 1)
        def _():
            out_sum(i - 2)

        @pl.when(i < NC)
        def _():
            got(i, 4)
            got(i, 5)
            pass_copy(i, 12).start()
            pass_copy(i, 13).start()

        @pl.when(jnp.logical_and(i > 0, i < NC))
        def _():
            work_b(i - 1)

        @pl.when(i < NC)
        def _():
            for slot in range(6, 14):
                got(i, slot)

        return carry

    lax.fori_loop(0, NC + 1, step, 0)

    def mate_copy(ph):
        return send(proj.at[ph, 1 - c], pbuf.at[ph], ars.at[ph, 0], arr.at[ph, 0], dp, mate)

    def rs_copy(ph, t):
        return send(rsb.at[ph, dp_at(t)], rcv.at[ph, dp], ars.at[ph, t], arr.at[ph, t], dp_at(t), mp)

    def y_copy(ph, t):
        to = ((y + t) % N_Y) * 2 + c
        return send(ysend.at[ph], ybuf.at[ph, y], ars.at[ph, 15 + t], arr.at[ph, 15 + t], dp, to)

    def ag_copy(ph, t):
        return send(agb.at[ph, dp], agb.at[ph, dp], ars.at[ph, 18 + t], arr.at[ph, 18 + t], dp_at(t), mp)

    def big_copy(ph):
        return send(bigf.at[ph, c], bigf.at[ph, c], ars.at[ph, 34], arr.at[ph, 34], dp, mate)

    def reduce_start(ph):
        mate_copy(ph).start()

    def reduce_scatter(ph):
        mate_copy(ph).wait_recv()
        own = proj[ph, c] + pbuf[ph]
        sm = small[ph]
        for j in range(N_DP):
            rsb[ph, j, 0:4] = own[4 * j : 4 * j + 4]
            rsb[ph, j, 4:8] = sm[4 * j : 4 * j + 4]
        for t in range(1, N_DP):
            rs_copy(ph, t).start()
        rcv[ph, dp] = rsb[ph, dp]

    def reduce_y(ph):
        for t in range(1, N_DP):
            rs_copy(ph, t).wait_recv()
        total = rcv[ph, 0]
        for j in range(1, N_DP):
            total = total + rcv[ph, j]
        ysend[ph] = total
        for t in range(1, N_Y):
            y_copy(ph, t).start()
        ybuf[ph, y] = total

    def gather_start(ph):
        for t in range(1, N_Y):
            y_copy(ph, t).wait_recv()
        total = ybuf[ph, 0]
        for j in range(1, N_Y):
            total = total + ybuf[ph, j]
        agb[ph, dp, 0:4] = total[0:4]
        agb[ph, dp, 4:8] = ysend[ph, 4:8]
        for t in range(1, N_DP):
            ag_copy(ph, t).start()

    def gather_mate(ph):
        for t in range(1, N_DP):
            ag_copy(ph, t).wait_recv()
        for j in range(N_DP):
            bigf[ph, c, 4 * j : 4 * j + 4] = agb[ph, j, 0:4]
            small[ph, 4 * j : 4 * j + 4] = agb[ph, j, 4:8]
        big_copy(ph).start()

    def gather_end(ph):
        big_copy(ph).wait_recv()
        return jnp.concatenate([bigf[ph, 0], bigf[ph, 1]], axis=1), small[ph]

    def piece(first, owner):
        at = pl.multiple_of((owner // 2) * feats, 32)
        return osb.at[pl.ds(first, HALF), pl.ds(at, feats), :]

    def y_first(k):
        src, dst, to = (
            (piece(0, far), ra, left), (piece(HALF, far), rb, right),
            (piece(0, right), da, right), (piece(HALF, left), db, left),
        )[k]
        return send(src, dst, ys.at[k], yr.at[k], dp, to)

    def y_second(k):
        src, dst, to = ((fa, ea, left), (fb, eb, right))[k]
        return send(src, dst, ys.at[4 + k], yr.at[4 + k], dp, to)

    def own_rows(i, owner):
        return osb[i, pl.ds(pl.multiple_of((owner // 2) * feats, 32), feats), :]

    def out_copy_dp(t, k):
        to = dp_at(t)
        return send(a2s.at[to, k], a2r.at[dp, k], a2ss.at[k, t], a2rr.at[k, t], to, mp)

    def gram_copy(t):
        return send(gbuf.at[mp], gbuf.at[mp], gms.at[t], gmr.at[t], dp, mp_at(t))

    reduce_start(0)
    work_b(NC - 1)
    reduce_scatter(0)
    out_sum(NC - 1)
    for k in range(4):
        y_first(k).start()
    reduce_y(0)
    for k in range(2):
        y_first(k).wait_recv()
    for i in range(HALF):
        fa[i] = (own_rows(i, left).astype(F32) + ra[i].astype(F32)).astype(BF16)
        fb[i] = (own_rows(HALF + i, right).astype(F32) + rb[i].astype(F32)).astype(BF16)
    gather_start(0)
    for k in range(2):
        y_second(k).start()
    gather_mate(0)
    proj_up, proj_down = gather_end(0)
    gram_d = gram_of(proj_down)
    gbuf[mp] = jnp.concatenate([gram_d, jnp.zeros_like(gram_d)], axis=1)
    for t in range(1, N_MP):
        gram_copy(t).start()
    quh[:, :half] = stack2(proj_down)
    qdh[...] = stack2(proj_up)

    def fresh(i, carry):
        add_projection(1, i, qdh[...], quh[...])
        return carry

    lax.fori_loop(0, NC, fresh, 0)
    reduce_start(1)
    for k in range(2, 4):
        y_first(k).wait_recv()
    for k in range(2):
        y_second(k).wait_recv()
    reduce_scatter(1)
    per = tc // BLOCK
    for i in range(NC):
        direct, summed = (da, ea) if i < HALF else (db, eb)
        j = i % HALF
        total = own_rows(i, mp).astype(F32) + direct[j].astype(F32) + summed[j].astype(F32)
        total = jnp.where(keep[i] > 0, total, 0.0).astype(BF16)
        for b in range(per):
            ob[i * per + b] = total[:, b * BLOCK : (b + 1) * BLOCK]
    for j in range(N_DP):
        for k in range(CAP):
            a2s[j, k] = ob[slot_idx[j * CAP + k]]
    for k in range(CAP):
        for t in range(1, N_DP):
            out_copy_dp(t, k).start()
    a2r[dp] = a2s[dp]
    for t in range(1, N_MP):
        gram_copy(t).wait_recv()
    total_gram = gbuf[0]
    for j in range(1, N_MP):
        total_gram = total_gram + gbuf[j]
    grams = jnp.stack([gram_of(proj_up), total_gram[:, :RANK]])
    inv = inverse_factors(grams)
    inv_u, inv_d = left3(inv[0].T), left3(inv[1].T)
    a3u[...] = left3(mm_tn(inv_u, right3(proj_up)))
    a3d[...] = left3(mm_tn(inv_d, right3(proj_down)))
    reduce_y(1)
    gather_start(1)
    gather_mate(1)
    fresh_down, fresh_up = gather_end(1)
    new_u = mm_tn(inv_u, right3(fresh_up))
    new_d = mm_tn(inv_d, right3(fresh_down))
    qnu[...] = new_u
    qnd[...] = new_d
    b3u[...] = right3(new_u)
    b3d[...] = right3(new_d)
    for k in range(CAP):
        for t in range(1, N_DP):
            out_copy_dp(t, k).wait_recv()
    for t in range(1, N_DP):
        send(er, erb.at[dp], ers.at[t], err_.at[t], dp_at(t), mp).wait()
    era_out[...] = erb[...]
    for j in range(N_DP):
        for k in range(CAP):
            a2o[j * CAP + k] = a2r[j, k]

    def sent(i, carry):
        for slot in range(14):
            (own_copy if slot in (0, 1, 2, 3, 6, 7) else pass_copy)(i, slot).wait_send()
        out_copy(i).wait_send()
        return carry

    lax.fori_loop(0, NC, sent, 0)
    for ph in range(2):
        mate_copy(ph).wait_send()
        big_copy(ph).wait_send()
        for t in range(1, N_Y):
            y_copy(ph, t).wait_send()
        for t in range(1, N_DP):
            rs_copy(ph, t).wait_send()
            ag_copy(ph, t).wait_send()
    for k in range(4):
        y_first(k).wait_send()
    for k in range(2):
        y_second(k).wait_send()
    for k in range(CAP):
        for t in range(1, N_DP):
            out_copy_dp(t, k).wait_send()
    for t in range(1, N_MP):
        gram_copy(t).wait_send()


def layer_kernel(slot_idx, xin, cin, wu, wd, qu, qd, er, keep):
    _, feats, tc = xin.shape
    width, ff = wu.shape
    half = width // 2
    vm = pl.BlockSpec(memory_space=pltpu.VMEM)
    shape = jax.ShapeDtypeStruct
    outs = [
        shape((N_DP * CAP, feats, BLOCK), BF16),
        shape((N_DP, 8, 128), jnp.int32),
        shape((3 * RANK, width), BF16),
        shape((3 * RANK, ff), BF16),
        shape((3 * RANK, ff), BF16),
        shape((3 * RANK, width), BF16),
        shape((RANK, ff), F32),
        shape((RANK, width), F32),
    ]
    dma = pltpu.SemaphoreType.DMA
    scratch = [
        pltpu.VMEM((NC, width, tc), BF16),
        pltpu.VMEM((NC, width, tc), BF16),
        pltpu.VMEM((NC, ff, tc), BF16),
        pltpu.VMEM((NC, ff, tc), BF16),
        pltpu.VMEM((ff, width), BF16),
        pltpu.VMEM((width, ff), BF16),
        pltpu.VMEM((2 * RANK, ff), BF16),
        pltpu.VMEM((2 * RANK, width), BF16),
        pltpu.VMEM((2, 2, RANK, half), F32),
        pltpu.VMEM((2, RANK, ff), F32),
        pltpu.VMEM((2, RANK, half), F32),
        pltpu.VMEM((2, N_DP, 8, half), F32),
        pltpu.VMEM((2, N_DP, 8, half), F32),
        pltpu.VMEM((2, 8, half), F32),
        pltpu.VMEM((2, N_Y, 8, half), F32),
        pltpu.VMEM((2, N_DP, 8, half), F32),
        pltpu.VMEM((2, 2, RANK, half), F32),
        pltpu.VMEM((N_MP, RANK, 128), F32),
        pltpu.VMEM((NC, 2, N_Y * feats, tc), BF16),
        pltpu.VMEM((NC, N_Y * feats, tc), BF16),
        pltpu.VMEM((NC, N_Y * feats, tc), BF16),
    ]
    scratch += [pltpu.VMEM((HALF, feats, tc), BF16) for _ in range(8)]
    scratch += [
        pltpu.VMEM((NC * tc // BLOCK, feats, BLOCK), BF16),
        pltpu.VMEM((N_DP, CAP, feats, BLOCK), BF16),
        pltpu.VMEM((N_DP, CAP, feats, BLOCK), BF16),
        pltpu.VMEM((N_DP, 8, 128), jnp.int32),
        dma((NC, 14)),
        dma((NC, 14)),
        dma((NC,)),
        dma((NC,)),
        dma((6,)),
        dma((6,)),
        dma((2, 35)),
        dma((2, 35)),
        dma((N_MP,)),
        dma((N_MP,)),
        dma((N_DP,)),
        dma((N_DP,)),
        dma((CAP, N_DP)),
        dma((CAP, N_DP)),
    ]
    return pl.pallas_call(
        kernel_body,
        out_shape=outs,
        in_specs=[pl.BlockSpec(memory_space=pltpu.SMEM)] + [vm] * 8,
        out_specs=[vm] * len(outs),
        scratch_shapes=scratch,
        compiler_params=pltpu.CompilerParams(
            collective_id=0, has_side_effects=True, vmem_limit_bytes=60 * 1024 * 1024
        ),
        name="layer",
    )(slot_idx, xin, cin, wu, wd, qu, qd, er, keep)


def place_body(ranks, blocks, out):
    me = lax.axis_index("dp")
    per = ranks.shape[1]

    out[...] = jnp.zeros_like(out)

    def source(r, filled):
        seen = jnp.int32(0)
        for b in range(per):
            mine = ranks[r, b] == me

            @pl.when(mine)
            def _(seen=seen, filled=filled):
                out[filled] = blocks[r * CAP + seen]

            step = mine.astype(jnp.int32)
            seen = seen + step
            filled = filled + step
        return filled

    lax.fori_loop(0, N_DP, source, jnp.int32(0))


def place(ranks, blocks):
    return pl.pallas_call(
        place_body,
        out_shape=jax.ShapeDtypeStruct((RMAX, *blocks.shape[1:]), blocks.dtype),
        in_specs=[
            pl.BlockSpec(memory_space=pltpu.SMEM),
            pl.BlockSpec(memory_space=pltpu.VMEM),
        ],
        out_specs=pl.BlockSpec(memory_space=pltpu.VMEM),
        name="place",
    )(ranks, blocks)


def send_slots(ranks):
    count = ranks.shape[0]
    ids = jnp.arange(count, dtype=jnp.int32)
    before = (ranks[None, :] == ranks[:, None]) & (ids[None, :] < ids[:, None])
    target = ranks * CAP + jnp.sum(before.astype(jnp.int32), axis=1)
    places = jnp.arange(N_DP * CAP, dtype=jnp.int32)
    return jnp.sum(jnp.where(places[:, None] == target[None, :], ids[None, :], 0), axis=1).astype(jnp.int32)


def chunked(rows):
    tokens, feats = rows.shape
    return rows.reshape(NC, tokens // NC, feats).transpose(0, 2, 1)


def local(patches, cotangent, encoder_rank, block_fill, w_up, w_down, q_up, q_down):
    tokens, feats = patches.shape
    blocks = encoder_rank.shape[0]
    within = jnp.arange(BLOCK, dtype=jnp.int32)
    kept = within[None, :] < block_fill[:, None]
    masked = jnp.where(kept.reshape(-1, 1), cotangent, jnp.zeros((), BF16))
    keep = kept.astype(F32).reshape(NC, 1, tokens // NC)
    er = jnp.broadcast_to(jnp.pad(encoder_rank, (0, 128 - blocks))[None, :], (8, 128))
    landed, ranks, a3u, b3u, a3d, b3d, qnu, qnd = layer_kernel(
        send_slots(encoder_rank), chunked(patches), chunked(masked), w_up, w_down,
        q_up.T, q_down.T, er, keep,
    )
    placed = place(ranks[:, 0, :blocks], landed)
    encoded = placed.transpose(0, 2, 1).reshape(RMAX * BLOCK, feats)
    approx_up = mm_tn(a3u, b3u)
    approx_down = mm_tn(a3d, b3d)
    return (encoded, approx_up, approx_down, qnu.T, qnd.T)


def solution(mesh):
    in_specs = (
        P("dp", "mp"), P("dp", "mp"), P("dp"), P("dp"), P(None, "mp"), P("mp", None), P("mp", None), P(),
    )
    out_specs = (P("dp", "mp"), P(None, "mp"), P("mp", None), P("mp", None), P())
    return jax.shard_map(local, mesh=mesh, in_specs=in_specs, out_specs=out_specs, check_vma=False)
```

```python
import jax
import jax.numpy as jnp
from jax import lax
from jax.experimental import pallas as pl
from jax.experimental.pallas import tpu as pltpu
from jax.sharding import PartitionSpec as P

BLOCK = 128
CAP = 2
RMAX = 18
BLK_DEV = 12
N_DP = 16
N_Y = 4
N_MP = 8
RANK = 64
NC = 6
HALF = NC // 2
AHEAD = 2
MESH = pl.DeviceIdType.MESH
F32 = jnp.float32
BF16 = jnp.bfloat16
NT = (((1,), (1,)), ((), ()))
TN = (((0,), (0,)), ((), ()))


def mm(a, b):
    return jnp.dot(a, b, preferred_element_type=F32)


def mm_nt(a, b):
    return lax.dot_general(a, b, NT, preferred_element_type=F32)


def mm_tn(a, b):
    return lax.dot_general(a, b, TN, preferred_element_type=F32)


def parts(v):
    hi = v.astype(BF16)
    lo = (v - hi.astype(F32)).astype(BF16)
    return hi, lo


def stack2(v):
    return jnp.concatenate(parts(v), axis=0)


def fold2(v):
    return v[:RANK] + v[RANK:]


def left4(v):
    hi, lo = parts(v)
    return jnp.concatenate([hi, hi, lo, lo], axis=0)


def right4(v):
    hi, lo = parts(v)
    return jnp.concatenate([hi, lo, hi, lo], axis=0)


def gram_of(v):
    s = stack2(v)
    g = mm_nt(s, s)
    return g[:RANK, :RANK] + g[:RANK, RANK:] + g[RANK:, :RANK] + g[RANK:, RANK:]


def eliminate(w, first, last):
    row = lax.broadcasted_iota(jnp.int32, w.shape, 1)
    for k in range(first, last):
        pivot = w[:, k : k + 1, k : k + 1]
        line = w[:, k : k + 1, :] * (1.0 / pivot)
        w = w - jnp.where(row > k, w[:, :, k : k + 1] * line, 0.0)
    return w


def identity_at_right(shape):
    row = lax.broadcasted_iota(jnp.int32, shape, 0)
    lane = lax.broadcasted_iota(jnp.int32, shape, 1)
    return jnp.where(lane == row + RANK, 1.0, 0.0).astype(F32)


def inverse_of_factor(w):
    row = lax.broadcasted_iota(jnp.int32, w.shape, 0)
    lane = lax.broadcasted_iota(jnp.int32, w.shape, 1)
    diag = jnp.sum(jnp.where(lane == row, w, 0.0), axis=1, keepdims=True)
    return (w * lax.rsqrt(diag))[:, RANK:]


def kernel_body(
    ranks, fills, pt, ct, wu, wd, qu, qd,
    a2o, a4u, a4d, era_out, qnu, qnd,
    xall, call, hid, gp, wus, wds, qus, qds, wut, wdt, quh, qdh,
    proj, small, pbuf, rsb, rcv, ysend, ybuf, agb, bigf, elim,
    gbuf, outp, po, osb, ra, rb, da, db, fa, fb, ea, eb, ob, a2s, f4u, f4d, ers, erb,
    lsem, nsem, msem, gsem, osem, ossem, ysem, yssem, arr, ars, mrr, mrs, xr, xs, a2rr, a2ss,
):
    dp = lax.axis_index("dp")
    mp = lax.axis_index("mp")
    y = mp // 2
    c = mp % 2
    right = ((y + 1) % N_Y) * 2 + c
    left = ((y + 3) % N_Y) * 2 + c
    far = ((y + 2) % N_Y) * 2 + c
    mate = y * 2 + (1 - c)
    feats = pt.shape[0]
    tc = xall.shape[2]
    per = tc // BLOCK
    blocks = NC * per
    half = proj.shape[3]

    def send(src, dst, ssem, rsem, dpi, mpi):
        return pltpu.make_async_remote_copy(
            src_ref=src, dst_ref=dst, send_sem=ssem, recv_sem=rsem,
            device_id=(dpi, mpi), device_id_type=MESH,
        )

    def arrived(ref, sem):
        send(ref, ref, sem, sem, dp, mate).wait_recv()

    def left_here(ref, sem):
        send(ref, ref, sem, sem, dp, mate).wait_send()

    def fetched(ref, sem):
        pltpu.make_async_copy(ref, ref, sem).wait()

    def dp_at(t):
        return (dp + t) % N_DP

    def mp_at(t):
        return (mp + t) % N_MP

    def rows(ref, i, owner):
        return ref.at[i, pl.ds(pl.multiple_of(owner * feats, 32), feats), :]

    barrier = pltpu.get_barrier_semaphore()
    for t in range(1, N_DP):
        pl.semaphore_signal(barrier, inc=1, device_id=(dp_at(t), mp), device_id_type=MESH)
    for t in range(1, N_MP):
        pl.semaphore_signal(barrier, inc=1, device_id=(dp, mp_at(t)), device_id_type=MESH)

    for i in range(NC):
        pltpu.make_async_copy(ct.at[:, pl.ds(i * tc, tc)], rows(call, i, mp), lsem.at[0]).start()
    for i in range(NC):
        pltpu.make_async_copy(pt.at[:, pl.ds(i * tc, tc)], rows(xall, i, mp), lsem.at[1]).start()
    weights = ((wu, wus), (wd, wds), (qu, qus), (qd, qds))
    for k, (src, dst) in enumerate(weights):
        pltpu.make_async_copy(src, dst, lsem.at[2 + k]).start()
    lane8 = lax.broadcasted_iota(jnp.int32, (8, 128), 1)
    mine = jnp.zeros((8, 128), jnp.int32)
    for b in range(blocks):
        mine = jnp.where(lane8 == b, ranks[b], mine)
    ers[...] = mine
    erb[dp] = mine
    token = lax.broadcasted_iota(jnp.int32, (feats, BLOCK), 1)
    def mask_cot(i):
        place_at = pl.ds(pl.multiple_of(mp * feats, 32), feats)
        for k in range(per):
            lanes = slice(k * BLOCK, (k + 1) * BLOCK)
            kept = jnp.where(token < fills[i * per + k], call[i, place_at, lanes].astype(F32), 0.0)
            call[i, place_at, lanes] = kept.astype(BF16)

    fetched(call.at[0, pl.ds(0, NC * feats), :], lsem.at[0])
    for i in range(AHEAD):
        mask_cot(i)
    fetched(xall.at[0, pl.ds(0, NC * feats), :], lsem.at[1])
    pl.semaphore_wait(barrier, N_DP + N_MP - 2)

    def pass_on(ref, which, i, owner, to, rsem):
        send(rows(ref, i, owner), rows(ref, i, owner), gsem.at[which], rsem, dp, to).start()

    def start_own(i):
        pass_on(xall, 0, i, mp, right, nsem.at[i, 0])
        pass_on(call, 1, i, mp, left, nsem.at[i, 0])
        pass_on(call, 1, i, mp, right, nsem.at[i, 1])
        pass_on(xall, 0, i, mp, left, nsem.at[i, 1])

    def pair(i):
        return xall.at[i, pl.ds(0, 2 * feats), :]

    for i in range(AHEAD):
        start_own(i)
    for i in range(AHEAD, NC):
        mask_cot(i)
    for i in range(NC):
        pass_on(xall, 0, i, mp, mate, msem.at[i])
        pass_on(call, 1, i, mp, mate, msem.at[i])
    for t in range(1, N_DP):
        send(ers, erb.at[dp], xs.at[0], xr.at[0], dp_at(t), mp).start()

    for k, (src, dst) in enumerate(weights):
        fetched(dst, lsem.at[2 + k])
    for j in range(wus.shape[1] // 128):
        wut[j * 128 : (j + 1) * 128, :] = wus[:, j * 128 : (j + 1) * 128].T
    for j in range(wds.shape[1] // 128):
        wdt[j * 128 : (j + 1) * 128, :] = wds[:, j * 128 : (j + 1) * 128].T
    quh[...] = stack2(qus[...])
    qdh[...] = stack2(qds[...])
    for ph in range(2):
        proj[ph] = jnp.zeros_like(proj[ph])
        small[ph] = jnp.zeros_like(small[ph])

    def start_out(i):
        send(outp.at[i, 1 - c], po.at[i], ossem.at[0], osem.at[i], dp, mate).start()

    def out_sum(i):
        arrived(po.at[i], osem.at[i])
        osb[i] = (outp[i, c].astype(F32) + po[i].astype(F32)).astype(BF16)

    def work_a(i):
        pre = mm(wut[...], xall[i])
        grad = mm(wds[...], call[i])
        sig = jax.nn.sigmoid(1.702 * pre)
        act = pre * sig
        hid[i] = act.astype(BF16)
        gp[i] = (grad * (sig + 1.702 * act * (1.0 - sig))).astype(BF16)

    def work_b(i):
        o = mm(wdt[...], hid[i]).astype(BF16)
        for m in range(N_MP):
            at = (m // 2) * feats
            outp[i, m % 2, at : at + feats, :] = o[m * feats : (m + 1) * feats]
        start_out(i)

    def big_add(ph, rows64, other):
        big = fold2(mm_nt(stack2(rows64), other))
        proj[ph, 0] += big[:, :half]
        proj[ph, 1] += big[:, half:]

    def small_add(ph, rows64, other):
        small[ph] += fold2(mm_nt(stack2(rows64), other))

    def add_projection(i):
        big_add(0, fold2(mm(quh[...], gp[i])), xall[i])
        small_add(0, fold2(mm(qdh[...], call[i])), hid[i])

    def piece(first, owner):
        at = pl.multiple_of((owner // 2) * feats, 32)
        return osb.at[pl.ds(first, HALF), pl.ds(at, feats), :]

    def own_rows(i, owner):
        return osb[i, pl.ds(pl.multiple_of((owner // 2) * feats, 32), feats), :]

    def send_b(i):
        j = i - HALF
        y_send(osb.at[i, pl.ds(pl.multiple_of((far // 2) * feats, 32), feats), :], rb.at[j], 1, right)
        y_send(osb.at[i, pl.ds(pl.multiple_of((left // 2) * feats, 32), feats), :], db.at[j], 5, left)

    def y_send(src, dst, group, to):
        send(src, dst, yssem.at[group], ysem.at[group], dp, to).start()

    def step(i, carry):
        @pl.when(i < NC)
        def _():
            arrived(pair(i), nsem.at[i, 0])
            pass_on(xall, 0, i, left, right, nsem.at[i, 2])
            pass_on(call, 1, i, right, left, nsem.at[i, 2])

            @pl.when(i + AHEAD < NC)
            def _():
                start_own(i + AHEAD)

            pass_on(xall, 0, i, left, mate, msem.at[i])
            pass_on(call, 1, i, right, mate, msem.at[i])

        @pl.when(i > 1)
        def _():
            arrived(xall.at[i - 2], msem.at[i - 2])
            work_a(i - 2)

        @pl.when(i < NC)
        def _():
            arrived(pair(i), nsem.at[i, 1])
            pass_on(call, 1, i, left, mate, msem.at[i])
            pass_on(xall, 0, i, right, mate, msem.at[i])

        @pl.when(i > 1)
        def _():
            add_projection(i - 2)

        @pl.when(jnp.logical_and(i > 2, i <= NC))
        def _():
            out_sum(i - 3)

        @pl.when(i == NC)
        def _():
            y_send(piece(0, far), ra, 0, left)
            y_send(piece(0, right), da, 4, right)
            send_b(HALF)

        @pl.when(jnp.logical_and(i > 0, i <= NC))
        def _():
            arrived(pair(i - 1), nsem.at[i - 1, 2])
            pass_on(xall, 0, i - 1, far, mate, msem.at[i - 1])
            pass_on(call, 1, i - 1, far, mate, msem.at[i - 1])

        @pl.when(jnp.logical_and(i > 1, i < NC))
        def _():
            work_b(i - 2)

        return carry

    lax.fori_loop(0, NC + 2, step, 0)

    def mate_start(ph):
        send(proj.at[ph, 1 - c], pbuf.at[ph], mrs.at[ph, 0], mrr.at[ph, 0], dp, mate).start()

    def mate_end(ph):
        arrived(pbuf.at[ph], mrr.at[ph, 0])
        return proj[ph, c] + pbuf[ph]

    def scatter(q, value):
        for j in range(N_DP):
            rsb[q, j] = value[4 * j : 4 * j + 4]
        for t in range(1, N_DP):
            to = dp_at(t)
            send(rsb.at[q, to], rcv.at[q, dp], ars.at[q, 0], arr.at[q, 0], to, mp).start()
        rcv[q, dp] = rsb[q, dp]

    def collect(q):
        arrived(rcv.at[q, pl.ds(0, N_DP - 1)], arr.at[q, 0])
        total = rcv[q, 0]
        for j in range(1, N_DP):
            total = total + rcv[q, j]
        return total

    def y_start(ph, q, total):
        ysend[ph] = total
        for t in range(1, N_Y):
            to = ((y + t) % N_Y) * 2 + c
            send(ysend.at[ph], ybuf.at[ph, y], ars.at[q, 2], arr.at[q, 2], dp, to).start()
        ybuf[ph, y] = total

    def y_end(ph, q):
        arrived(ybuf.at[ph, pl.ds(0, N_Y - 1)], arr.at[q, 2])
        total = ybuf[ph, 0]
        for j in range(1, N_Y):
            total = total + ybuf[ph, j]
        return total

    def spread(q, total):
        agb[q, dp] = total
        for t in range(1, N_DP):
            send(agb.at[q, dp], agb.at[q, dp], ars.at[q, 1], arr.at[q, 1], dp_at(t), mp).start()

    def small_end(ph, q):
        arrived(agb.at[q, pl.ds(0, N_DP - 1)], arr.at[q, 1])
        for j in range(N_DP):
            small[ph, 4 * j : 4 * j + 4] = agb[q, j]
        return small[ph]

    def big_start(ph, q):
        arrived(agb.at[q, pl.ds(0, N_DP - 1)], arr.at[q, 1])
        for j in range(N_DP):
            bigf[ph, c, 4 * j : 4 * j + 4] = agb[q, j]
        send(bigf.at[ph, c], bigf.at[ph, c], mrs.at[ph, 1], mrr.at[ph, 1], dp, mate).start()

    def big_end(ph):
        arrived(bigf.at[ph, 0], mrr.at[ph, 1])
        return jnp.concatenate([bigf[ph, 0], bigf[ph, 1]], axis=1)

    def start_slots(k, first, last):
        for t in range(first, last):
            to = dp_at(t)
            send(a2s.at[k, to], a2o.at[k, dp], a2ss.at[k], a2rr.at[k], to, mp).start()

    def out_landed(k):
        arrived(a2o.at[k, pl.ds(0, N_DP - 1)], a2rr.at[k])

    mate_start(0)
    scatter(1, small[0])
    work_b(NC - 2)
    scatter(0, mate_end(0))
    work_b(NC - 1)
    for i in range(HALF + 1, NC):
        out_sum(i)
        send_b(i)
    arrived(ra, ysem.at[0])
    for i in range(HALF):
        fa[i] = (own_rows(i, left).astype(F32) + ra[i].astype(F32)).astype(BF16)
    spread(1, collect(1))
    y_start(0, 0, collect(0))
    y_send(fa, ea, 2, left)
    spread(0, y_end(0, 0))
    arrived(rb, ysem.at[1])
    for i in range(HALF):
        fb[i] = (own_rows(HALF + i, right).astype(F32) + rb[i].astype(F32)).astype(BF16)
    y_send(fb, eb, 3, right)
    proj_down = small_end(0, 1)
    quh[:, :half] = stack2(proj_down)

    def fresh_down(i, carry):
        big_add(1, fold2(mm(quh[...], hid[i])), call[i])
        return carry

    lax.fori_loop(0, NC, fresh_down, 0)
    mate_start(1)
    gram_d = gram_of(proj_down)
    gbuf[mp] = jnp.concatenate([gram_d[: RANK // 2], gram_d[RANK // 2 :]], axis=1)
    for t in range(1, N_MP):
        send(gbuf.at[mp], gbuf.at[mp], xs.at[1], xr.at[1], dp, mp_at(t)).start()
    big_start(0, 0)
    scatter(2, mate_end(1))
    proj_up = big_end(0)
    qdh[...] = stack2(proj_up)

    def fresh_up(i, carry):
        small_add(1, fold2(mm(qdh[...], xall[i])), gp[i])
        return carry

    lax.fori_loop(0, HALF, fresh_up, 0)
    arrived(ea, ysem.at[2])
    arrived(eb, ysem.at[3])
    arrived(da, ysem.at[4])
    arrived(db, ysem.at[5])
    for b in range(blocks):
        i, at = b // per, (b % per) * BLOCK
        direct, summed = (da, ea) if i < HALF else (db, eb)
        lanes = slice(at, at + BLOCK)
        total = own_rows(i, mp)[:, lanes].astype(F32)
        total = total + direct[i % HALF, :, lanes].astype(F32) + summed[i % HALF, :, lanes].astype(F32)
        ob[b] = jnp.where(token < fills[b], total, 0.0).astype(BF16)
    for j in range(N_DP):
        first = jnp.int32(0)
        second = jnp.int32(0)
        for b in range(blocks - 1, -1, -1):
            here = ranks[b] == j
            second = jnp.where(here, first, second)
            first = jnp.where(here, b, first)
        a2s[0, j] = ob[first]
        a2s[1, j] = ob[second]
    start_slots(0, 1, 8)
    for k in range(CAP):
        pltpu.make_async_copy(a2s.at[k, dp], a2o.at[k, dp], lsem.at[k]).start()
    lax.fori_loop(HALF, NC, fresh_up, 0)
    scatter(3, small[1])
    start_slots(0, 8, N_DP)
    y_start(1, 2, collect(2))
    elim[0] = identity_at_right((RANK, 2 * RANK))
    elim[0, :, :RANK] = gram_of(proj_up)
    arrived(gbuf.at[pl.ds(0, N_MP - 1)], xr.at[1])
    gram_d = gbuf[0]
    for j in range(1, N_MP):
        gram_d = gram_d + gbuf[j]
    elim[1] = identity_at_right((RANK, 2 * RANK))
    elim[1, : RANK // 2, :RANK] = gram_d[:, :RANK]
    elim[1, RANK // 2 :, :RANK] = gram_d[:, RANK:]
    elim[...] = eliminate(elim[...], 0, 8)
    spread(2, y_end(1, 2))
    start_slots(1, 1, 8)
    elim[...] = eliminate(elim[...], 8, 24)
    spread(3, collect(3))
    start_slots(1, 8, N_DP)
    elim[...] = eliminate(elim[...], 24, RANK - 1)
    inv_u = left4(inverse_of_factor(elim[0]).T)
    inv_d = left4(inverse_of_factor(elim[1]).T)
    f4u[...] = left4(mm_tn(inv_u, right4(proj_up))).T
    f4d[...] = left4(mm_tn(inv_d, right4(proj_down))).T
    pltpu.make_async_copy(f4u, a4u, lsem.at[2]).start()
    pltpu.make_async_copy(f4d, a4d, lsem.at[3]).start()
    arrived(erb.at[pl.ds(0, N_DP - 1)], xr.at[0])
    for r in range(N_DP):
        era_out[r : r + 1, :] = erb[r, 0:1, :]
    big_start(1, 2)
    out_landed(0)
    new_u = mm_tn(inv_u, right4(small_end(1, 3)))
    qnu[...] = new_u
    new_d = mm_tn(inv_d, right4(big_end(1)))
    qnd[...] = new_d
    out_landed(1)

    pltpu.make_async_copy(f4u, a4u, lsem.at[2]).wait()
    pltpu.make_async_copy(f4d, a4d, lsem.at[3]).wait()
    left_here(xall.at[:, pl.ds(0, 7 * feats), :], gsem.at[0])
    left_here(call.at[:, pl.ds(0, 7 * feats), :], gsem.at[1])
    left_here(po, ossem.at[0])
    left_here(erb.at[pl.ds(0, N_DP - 1)], xs.at[0])
    left_here(gbuf.at[pl.ds(0, N_MP - 1)], xs.at[1])
    for group, ref in enumerate((ra, rb, ea, eb, da, db)):
        left_here(ref, yssem.at[group])
    for ph in range(2):
        left_here(pbuf.at[ph], mrs.at[ph, 0])
        left_here(bigf.at[ph, 0], mrs.at[ph, 1])
        left_here(ybuf.at[ph, pl.ds(0, N_Y - 1)], ars.at[2 * ph, 2])
    for q in range(4):
        left_here(rcv.at[q, pl.ds(0, N_DP - 1)], ars.at[q, 0])
        left_here(agb.at[q, pl.ds(0, N_DP - 1)], ars.at[q, 1])
    for k in range(CAP):
        left_here(a2s.at[k, pl.ds(0, N_DP - 1)], a2ss.at[k])
        pltpu.make_async_copy(a2s.at[k, dp], a2o.at[k, dp], lsem.at[k]).wait()


def layer_kernel(ranks, fills, pt, ct, wu, wd, qu, qd):
    feats, tokens = pt.shape
    tc = tokens // NC
    width, ff = wu.shape
    half = width // 2
    vm = pl.BlockSpec(memory_space=pltpu.VMEM)
    sm = pl.BlockSpec(memory_space=pltpu.SMEM)
    anywhere = pl.BlockSpec(memory_space=pl.ANY)
    shape = jax.ShapeDtypeStruct
    outs = [
        shape((CAP, N_DP, feats, BLOCK), BF16),
        shape((width, 4 * RANK), BF16),
        shape((ff, 4 * RANK), BF16),
        shape((N_DP, 128), jnp.int32),
        shape((RANK, ff), F32),
        shape((RANK, width), F32),
    ]
    dma = pltpu.SemaphoreType.DMA
    scratch = [
        pltpu.VMEM((NC, width, tc), BF16),
        pltpu.VMEM((NC, width, tc), BF16),
        pltpu.VMEM((NC, ff, tc), BF16),
        pltpu.VMEM((NC, ff, tc), BF16),
        pltpu.VMEM((width, ff), BF16),
        pltpu.VMEM((ff, width), BF16),
        pltpu.VMEM((RANK, ff), F32),
        pltpu.VMEM((RANK, width), F32),
        pltpu.VMEM((ff, width), BF16),
        pltpu.VMEM((width, ff), BF16),
        pltpu.VMEM((2 * RANK, ff), BF16),
        pltpu.VMEM((2 * RANK, width), BF16),
        pltpu.VMEM((2, 2, RANK, half), F32),
        pltpu.VMEM((2, RANK, ff), F32),
        pltpu.VMEM((2, RANK, half), F32),
        pltpu.VMEM((4, N_DP, 4, half), F32),
        pltpu.VMEM((4, N_DP, 4, half), F32),
        pltpu.VMEM((2, 4, half), F32),
        pltpu.VMEM((2, N_Y, 4, half), F32),
        pltpu.VMEM((4, N_DP, 4, half), F32),
        pltpu.VMEM((2, 2, RANK, half), F32),
        pltpu.VMEM((2, RANK, 2 * RANK), F32),
        pltpu.VMEM((N_MP, RANK // 2, 2 * RANK), F32),
        pltpu.VMEM((NC, 2, N_Y * feats, tc), BF16),
        pltpu.VMEM((NC, N_Y * feats, tc), BF16),
        pltpu.VMEM((NC, N_Y * feats, tc), BF16),
    ]
    scratch += [pltpu.VMEM((HALF, feats, tc), BF16) for _ in range(8)]
    scratch += [
        pltpu.VMEM((tokens // BLOCK, feats, BLOCK), BF16),
        pltpu.VMEM((CAP, N_DP, feats, BLOCK), BF16),
        pltpu.VMEM((width, 4 * RANK), BF16),
        pltpu.VMEM((ff, 4 * RANK), BF16),
        pltpu.VMEM((8, 128), jnp.int32),
        pltpu.VMEM((N_DP, 8, 128), jnp.int32),
        dma((6,)),
        dma((NC, 3)),
        dma((NC,)),
        dma((2,)),
        dma((NC,)),
        dma((1,)),
        dma((6,)),
        dma((6,)),
        dma((4, 3)),
        dma((4, 3)),
        dma((2, 2)),
        dma((2, 2)),
        dma((2,)),
        dma((2,)),
        dma((CAP,)),
        dma((CAP,)),
    ]
    return pl.pallas_call(
        kernel_body,
        out_shape=outs,
        in_specs=[sm] * 2 + [anywhere] * 6,
        out_specs=[anywhere] * 3 + [vm] * 3,
        scratch_shapes=scratch,
        compiler_params=pltpu.CompilerParams(
            collective_id=0, has_side_effects=True, vmem_limit_bytes=60 * 1024 * 1024
        ),
        name="layer",
    )(ranks, fills, pt, ct, wu, wd, qu, qd)


def finish_body(
    ranks, landed, a4u, a4d, qnu, qnd,
    enc, up, down, new_u, new_d,
    blocks, placed, ups, downs, b4u, b4d, origin, sems,
):
    me = lax.axis_index("dp")
    for k in range(CAP):
        pltpu.make_async_copy(landed.at[k], blocks.at[pl.ds(k * N_DP, N_DP)], sems.at[10 + k]).start()
    for slot in range(RMAX + 1):
        origin[slot] = CAP * N_DP
    filled = jnp.int32(0)
    for r in range(N_DP):
        seen = jnp.int32(0)
        for b in range(BLK_DEV):
            hit = (ranks[r, b] == me).astype(jnp.int32)
            held = origin[filled]
            origin[filled] = jnp.where(hit > 0, seen * N_DP + r, held)
            seen = seen + hit
            filled = filled + hit
    copies = []
    b4u[...] = right4(qnu[...])
    b4d[...] = right4(qnd[...])
    for k, (a, b, stage, out) in enumerate(((a4u, b4u, ups, up), (a4d, b4d, downs, down))):
        pieces = 2
        size = stage.shape[0] // pieces
        for j in range(pieces):
            at = pl.ds(j * size, size)
            stage[at, :] = mm(a[at, :], b[...])
            copy = pltpu.make_async_copy(stage.at[at, :], out.at[at, :], sems.at[k * pieces + j])
            copy.start()
            copies.append(copy)
    new_u[...] = qnu[...]
    new_d[...] = qnd[...]
    blocks[CAP * N_DP] = jnp.zeros_like(blocks[CAP * N_DP])
    for k in range(CAP):
        pltpu.make_async_copy(landed.at[k], blocks.at[pl.ds(k * N_DP, N_DP)], sems.at[10 + k]).wait()
    for slot in range(RMAX):
        placed[:, slot * BLOCK : (slot + 1) * BLOCK] = blocks[origin[slot]]
    copy = pltpu.make_async_copy(placed, enc, sems.at[12])
    copy.start()
    copies.append(copy)
    for copy in copies:
        copy.wait()


def finish(landed, a4u, a4d, ranks, qnu, qnd):
    feats = landed.shape[2]
    width, ff = a4u.shape[0], a4d.shape[0]
    vm = pl.BlockSpec(memory_space=pltpu.VMEM)
    anywhere = pl.BlockSpec(memory_space=pl.ANY)
    shape = jax.ShapeDtypeStruct
    return pl.pallas_call(
        finish_body,
        out_shape=[
            shape((feats, RMAX * BLOCK), BF16),
            shape((width, ff), F32),
            shape((ff, width), F32),
            shape(qnu.shape, F32),
            shape(qnd.shape, F32),
        ],
        in_specs=[pl.BlockSpec(memory_space=pltpu.SMEM), anywhere] + [vm] * 4,
        out_specs=[anywhere] * 3 + [vm] * 2,
        scratch_shapes=[
            pltpu.VMEM((CAP * N_DP + 1, *landed.shape[2:]), BF16),
            pltpu.VMEM((feats, RMAX * BLOCK), BF16),
            pltpu.VMEM((width, ff), F32),
            pltpu.VMEM((ff, width), F32),
            pltpu.VMEM((4 * RANK, ff), BF16),
            pltpu.VMEM((4 * RANK, width), BF16),
            pltpu.SMEM((RMAX + 1,), jnp.int32),
            pltpu.SemaphoreType.DMA((13,)),
        ],
        name="finish",
    )(ranks, landed, a4u, a4d, qnu, qnd)


def local(patches, cotangent, encoder_rank, block_fill, w_up, w_down, q_up, q_down):
    results = layer_kernel(
        encoder_rank, block_fill, patches.T, cotangent.T, w_up, w_down, q_up.T, q_down.T
    )
    encoded, approx_up, approx_down, new_u, new_d = finish(*results)
    return (encoded.T, approx_up, approx_down, new_u.T, new_d.T)


def solution(mesh):
    in_specs = (
        P("dp", "mp"), P("dp", "mp"), P("dp"), P("dp"), P(None, "mp"), P("mp", None), P("mp", None), P(),
    )
    out_specs = (P("dp", "mp"), P(None, "mp"), P("mp", None), P("mp", None), P())
    return jax.shard_map(local, mesh=mesh, in_specs=in_specs, out_specs=out_specs, check_vma=False)
```

```python
import jax
import jax.numpy as jnp
from jax import lax
from jax.experimental import pallas as pl
from jax.experimental.pallas import tpu as pltpu
from jax.sharding import PartitionSpec as P

BLOCK = 128
CAP = 2
RMAX = 18
BLK_DEV = 12
N_DP = 16
N_Y = 4
N_MP = 8
GROUPS = ((1, 4, 10, 15), (2, 8, 7, 13), (3, 12, 5, 11), (6, 9, 14))
RANK = 64
NC = 6
HALF = NC // 2
AHEAD = 2
MESH = pl.DeviceIdType.MESH
F32 = jnp.float32
BF16 = jnp.bfloat16
NT = (((1,), (1,)), ((), ()))
TN = (((0,), (0,)), ((), ()))


def mm(a, b):
    return jnp.dot(a, b, preferred_element_type=F32)


def mm_nt(a, b):
    return lax.dot_general(a, b, NT, preferred_element_type=F32)


def mm_tn(a, b):
    return lax.dot_general(a, b, TN, preferred_element_type=F32)


def parts(v):
    hi = v.astype(BF16)
    lo = (v - hi.astype(F32)).astype(BF16)
    return hi, lo


def stack2(v):
    return jnp.concatenate(parts(v), axis=0)


def fold2(v):
    return v[:RANK] + v[RANK:]


def left4(v):
    hi, lo = parts(v)
    return jnp.concatenate([hi, hi, lo, lo], axis=0)


def right4(v):
    hi, lo = parts(v)
    return jnp.concatenate([hi, lo, hi, lo], axis=0)


def gram_of(v):
    s = stack2(v)
    g = mm_nt(s, s)
    return g[:RANK, :RANK] + g[:RANK, RANK:] + g[RANK:, :RANK] + g[RANK:, RANK:]


def eliminate(w, first, last):
    row = lax.broadcasted_iota(jnp.int32, w.shape, 1)
    for k in range(first, last):
        pivot = w[:, k : k + 1, k : k + 1]
        line = w[:, k : k + 1, :] * (1.0 / pivot)
        w = w - jnp.where(row > k, w[:, :, k : k + 1] * line, 0.0)
    return w


def identity_at_right(shape):
    row = lax.broadcasted_iota(jnp.int32, shape, 0)
    lane = lax.broadcasted_iota(jnp.int32, shape, 1)
    return jnp.where(lane == row + RANK, 1.0, 0.0).astype(F32)


def inverse_of_factor(w):
    row = lax.broadcasted_iota(jnp.int32, w.shape, 0)
    lane = lax.broadcasted_iota(jnp.int32, w.shape, 1)
    diag = jnp.sum(jnp.where(lane == row, w, 0.0), axis=1, keepdims=True)
    return (w * lax.rsqrt(diag))[:, RANK:]


def kernel_body(
    ranks, fills, pt, ct, wu, wd, qu, qd,
    a2o, a4u, a4d, era_out, qnu, qnd,
    xall, call, hid, gp, wus, wds, qus, qds, wut, wdt, quh, qdh,
    proj, small, pbuf, rsb, rcv, ysend, ybuf, agb, bigf, elim,
    gbuf, outp, po, osb, ra, rb, da, db, fa, fb, ea, eb, ob, a2s, f4u, f4d, ers, erb,
    lsem, nsem, msem, gsem, osem, ossem, ysem, yssem, arr, ars, mrr, mrs, xr, xs, a2rr, a2ss,
):
    dp = lax.axis_index("dp")
    mp = lax.axis_index("mp")
    y = mp // 2
    c = mp % 2
    right = ((y + 1) % N_Y) * 2 + c
    left = ((y + 3) % N_Y) * 2 + c
    far = ((y + 2) % N_Y) * 2 + c
    mate = y * 2 + (1 - c)
    feats = pt.shape[0]
    tc = xall.shape[2]
    per = tc // BLOCK
    blocks = NC * per
    half = proj.shape[3]

    def send(src, dst, ssem, rsem, dpi, mpi):
        return pltpu.make_async_remote_copy(
            src_ref=src, dst_ref=dst, send_sem=ssem, recv_sem=rsem,
            device_id=(dpi, mpi), device_id_type=MESH,
        )

    def arrived(ref, sem):
        send(ref, ref, sem, sem, dp, mate).wait_recv()

    def left_here(ref, sem):
        send(ref, ref, sem, sem, dp, mate).wait_send()

    def fetched(ref, sem):
        pltpu.make_async_copy(ref, ref, sem).wait()

    def dp_at(t):
        return ((dp // N_Y + t // N_Y) % N_Y) * N_Y + (dp + t) % N_Y

    def mp_at(t):
        return (mp + t) % N_MP

    def rows(ref, i, owner):
        return ref.at[i, pl.ds(pl.multiple_of(owner * feats, 32), feats), :]

    barrier = pltpu.get_barrier_semaphore()
    for t in range(1, N_DP):
        pl.semaphore_signal(barrier, inc=1, device_id=(dp_at(t), mp), device_id_type=MESH)
    for t in range(1, N_MP):
        pl.semaphore_signal(barrier, inc=1, device_id=(dp, mp_at(t)), device_id_type=MESH)

    for i in range(NC):
        pltpu.make_async_copy(ct.at[:, pl.ds(i * tc, tc)], rows(call, i, mp), lsem.at[0]).start()
    for i in range(NC):
        pltpu.make_async_copy(pt.at[:, pl.ds(i * tc, tc)], rows(xall, i, mp), lsem.at[1]).start()
    weights = ((wu, wus), (wd, wds), (qu, qus), (qd, qds))
    for k, (src, dst) in enumerate(weights):
        pltpu.make_async_copy(src, dst, lsem.at[2 + k]).start()
    lane8 = lax.broadcasted_iota(jnp.int32, (8, 128), 1)
    mine = jnp.zeros((8, 128), jnp.int32)
    for b in range(blocks):
        mine = jnp.where(lane8 == b, ranks[b], mine)
    ers[...] = mine
    erb[dp] = mine
    token = lax.broadcasted_iota(jnp.int32, (feats, BLOCK), 1)
    def mask_cot(i):
        place_at = pl.ds(pl.multiple_of(mp * feats, 32), feats)
        for k in range(per):
            lanes = slice(k * BLOCK, (k + 1) * BLOCK)
            kept = jnp.where(token < fills[i * per + k], call[i, place_at, lanes].astype(F32), 0.0)
            call[i, place_at, lanes] = kept.astype(BF16)

    fetched(call.at[0, pl.ds(0, NC * feats), :], lsem.at[0])
    for i in range(AHEAD):
        mask_cot(i)
    fetched(xall.at[0, pl.ds(0, NC * feats), :], lsem.at[1])
    pl.semaphore_wait(barrier, N_DP + N_MP - 2)

    def pass_on(ref, which, i, owner, to, rsem):
        send(rows(ref, i, owner), rows(ref, i, owner), gsem.at[which], rsem, dp, to).start()

    def start_own(i):
        pass_on(xall, 0, i, mp, right, nsem.at[i, 0])
        pass_on(call, 1, i, mp, left, nsem.at[i, 0])
        pass_on(call, 1, i, mp, right, nsem.at[i, 1])
        pass_on(xall, 0, i, mp, left, nsem.at[i, 1])

    def pair(i):
        return xall.at[i, pl.ds(0, 2 * feats), :]

    for i in range(AHEAD):
        start_own(i)
    for i in range(AHEAD, NC):
        mask_cot(i)
    for i in range(NC):
        pass_on(xall, 0, i, mp, mate, msem.at[i])
        pass_on(call, 1, i, mp, mate, msem.at[i])
    for t in range(1, N_DP):
        send(ers, erb.at[dp], xs.at[0], xr.at[0], dp_at(t), mp).start()

    for k, (src, dst) in enumerate(weights):
        fetched(dst, lsem.at[2 + k])
    for j in range(wus.shape[1] // 128):
        wut[j * 128 : (j + 1) * 128, :] = wus[:, j * 128 : (j + 1) * 128].T
    for j in range(wds.shape[1] // 128):
        wdt[j * 128 : (j + 1) * 128, :] = wds[:, j * 128 : (j + 1) * 128].T
    quh[...] = stack2(qus[...])
    qdh[...] = stack2(qds[...])
    for ph in range(2):
        proj[ph] = jnp.zeros_like(proj[ph])
        small[ph] = jnp.zeros_like(small[ph])

    def start_out(i):
        send(outp.at[i, 1 - c], po.at[i], ossem.at[0], osem.at[i], dp, mate).start()

    def out_sum(i):
        arrived(po.at[i], osem.at[i])
        osb[i] = (outp[i, c].astype(F32) + po[i].astype(F32)).astype(BF16)

    def work_a(i):
        pre = mm(wut[...], xall[i])
        grad = mm(wds[...], call[i])
        sig = jax.nn.sigmoid(1.702 * pre)
        act = pre * sig
        hid[i] = act.astype(BF16)
        gp[i] = (grad * (sig + 1.702 * act * (1.0 - sig))).astype(BF16)

    def work_b(i):
        o = mm(wdt[...], hid[i]).astype(BF16)
        for m in range(N_MP):
            at = (m // 2) * feats
            outp[i, m % 2, at : at + feats, :] = o[m * feats : (m + 1) * feats]
        start_out(i)

    def big_add(ph, rows64, other):
        big = fold2(mm_nt(stack2(rows64), other))
        proj[ph, 0] += big[:, :half]
        proj[ph, 1] += big[:, half:]

    def small_add(ph, rows64, other):
        small[ph] += fold2(mm_nt(stack2(rows64), other))

    def add_projection(i):
        big_add(0, fold2(mm(quh[...], gp[i])), xall[i])
        small_add(0, fold2(mm(qdh[...], call[i])), hid[i])

    def piece(first, owner):
        at = pl.multiple_of((owner // 2) * feats, 32)
        return osb.at[pl.ds(first, HALF), pl.ds(at, feats), :]

    def own_rows(i, owner):
        return osb[i, pl.ds(pl.multiple_of((owner // 2) * feats, 32), feats), :]

    def send_b(i):
        j = i - HALF
        y_send(osb.at[i, pl.ds(pl.multiple_of((far // 2) * feats, 32), feats), :], rb.at[j], 1, right)
        y_send(osb.at[i, pl.ds(pl.multiple_of((left // 2) * feats, 32), feats), :], db.at[j], 5, left)

    def y_send(src, dst, group, to):
        send(src, dst, yssem.at[group], ysem.at[group], dp, to).start()

    def mate_start(ph):
        send(proj.at[ph, 1 - c], pbuf.at[ph], mrs.at[ph, 0], mrr.at[ph, 0], dp, mate).start()

    def mate_end(ph):
        arrived(pbuf.at[ph], mrr.at[ph, 0])
        return proj[ph, c] + pbuf[ph]

    def scatter(q, value):
        for j in range(N_DP):
            rsb[q, j] = value[4 * j : 4 * j + 4]
        for t in range(1, N_DP):
            to = dp_at(t)
            send(rsb.at[q, to], rcv.at[q, dp], ars.at[q, 0], arr.at[q, 0], to, mp).start()
        rcv[q, dp] = rsb[q, dp]

    def collect(q):
        arrived(rcv.at[q, pl.ds(0, N_DP - 1)], arr.at[q, 0])
        total = rcv[q, 0]
        for j in range(1, N_DP):
            total = total + rcv[q, j]
        return total

    def y_start(ph, q, total):
        ysend[ph] = total
        for t in range(1, N_Y):
            to = ((y + t) % N_Y) * 2 + c
            send(ysend.at[ph], ybuf.at[ph, y], ars.at[q, 2], arr.at[q, 2], dp, to).start()
        ybuf[ph, y] = total

    def y_end(ph, q):
        arrived(ybuf.at[ph, pl.ds(0, N_Y - 1)], arr.at[q, 2])
        total = ybuf[ph, 0]
        for j in range(1, N_Y):
            total = total + ybuf[ph, j]
        return total

    def spread(q, total):
        agb[q, dp] = total
        for t in range(1, N_DP):
            send(agb.at[q, dp], agb.at[q, dp], ars.at[q, 1], arr.at[q, 1], dp_at(t), mp).start()

    def small_end(ph, q):
        arrived(agb.at[q, pl.ds(0, N_DP - 1)], arr.at[q, 1])
        for j in range(N_DP):
            small[ph, 4 * j : 4 * j + 4] = agb[q, j]
        return small[ph]

    def big_start(ph, q):
        arrived(agb.at[q, pl.ds(0, N_DP - 1)], arr.at[q, 1])
        for j in range(N_DP):
            bigf[ph, c, 4 * j : 4 * j + 4] = agb[q, j]
        send(bigf.at[ph, c], bigf.at[ph, c], mrs.at[ph, 1], mrr.at[ph, 1], dp, mate).start()

    def big_end(ph):
        arrived(bigf.at[ph, 0], mrr.at[ph, 1])
        return jnp.concatenate([bigf[ph, 0], bigf[ph, 1]], axis=1)

    def step(i, carry):
        @pl.when(i < NC)
        def _():
            arrived(pair(i), nsem.at[i, 0])
            pass_on(xall, 0, i, left, right, nsem.at[i, 2])
            pass_on(call, 1, i, right, left, nsem.at[i, 2])

            @pl.when(i + AHEAD < NC)
            def _():
                start_own(i + AHEAD)

            pass_on(xall, 0, i, left, mate, msem.at[i])
            pass_on(call, 1, i, right, mate, msem.at[i])

        @pl.when(jnp.logical_and(i > 1, i < NC + 2))
        def _():
            arrived(xall.at[i - 2], msem.at[i - 2])
            work_a(i - 2)

        @pl.when(i < NC)
        def _():
            arrived(pair(i), nsem.at[i, 1])
            pass_on(call, 1, i, left, mate, msem.at[i])
            pass_on(xall, 0, i, right, mate, msem.at[i])

        @pl.when(jnp.logical_and(i > 1, i < NC + 2))
        def _():
            add_projection(i - 2)

        @pl.when(jnp.logical_and(i > 2, i <= NC))
        def _():
            out_sum(i - 3)

        @pl.when(i == NC)
        def _():
            y_send(piece(0, far), ra, 0, left)
            y_send(piece(0, right), da, 4, right)
            send_b(HALF)

        @pl.when(jnp.logical_and(i > 0, i <= NC))
        def _():
            arrived(pair(i - 1), nsem.at[i - 1, 2])
            pass_on(xall, 0, i - 1, far, mate, msem.at[i - 1])
            pass_on(call, 1, i - 1, far, mate, msem.at[i - 1])

        @pl.when(i == NC + 3)
        def _():
            scatter(0, mate_end(0))

        @pl.when(jnp.logical_or(jnp.logical_and(i > 1, i < NC), i > NC + 1))
        def _():
            work_b(jnp.where(i < NC, i - 2, i - 4))

        @pl.when(i == NC + 1)
        def _():
            mate_start(0)
            scatter(1, small[0])

        return carry

    lax.fori_loop(0, NC + 4, step, 0)

    def start_slots(k, group):
        for t in GROUPS[group]:
            to = dp_at(t)
            send(a2s.at[k, to], a2o.at[k, dp], a2ss.at[k], a2rr.at[k], to, mp).start()

    def out_landed(k):
        arrived(a2o.at[k, pl.ds(0, N_DP - 1)], a2rr.at[k])

    for i in range(HALF + 1, NC):
        out_sum(i)
        send_b(i)
    arrived(ra, ysem.at[0])
    for i in range(HALF):
        fa[i] = (own_rows(i, left).astype(F32) + ra[i].astype(F32)).astype(BF16)
    spread(1, collect(1))
    y_start(0, 0, collect(0))
    y_send(fa, ea, 2, left)
    arrived(rb, ysem.at[1])
    for i in range(HALF):
        fb[i] = (own_rows(HALF + i, right).astype(F32) + rb[i].astype(F32)).astype(BF16)
    y_send(fb, eb, 3, right)
    spread(0, y_end(0, 0))
    proj_down = small_end(0, 1)
    quh[:, :half] = stack2(proj_down)

    def fresh_down(i, carry):
        big_add(1, fold2(mm(quh[...], hid[i])), call[i])
        return carry

    lax.fori_loop(0, NC, fresh_down, 0)
    mate_start(1)
    gram_d = gram_of(proj_down)
    gbuf[mp] = jnp.concatenate([gram_d[: RANK // 2], gram_d[RANK // 2 :]], axis=1)
    for t in range(1, N_MP):
        send(gbuf.at[mp], gbuf.at[mp], xs.at[1], xr.at[1], dp, mp_at(t)).start()
    big_start(0, 0)
    scatter(2, mate_end(1))
    arrived(ea, ysem.at[2])
    arrived(eb, ysem.at[3])
    arrived(da, ysem.at[4])
    arrived(db, ysem.at[5])
    for b in range(blocks):
        i, at = b // per, (b % per) * BLOCK
        direct, summed = (da, ea) if i < HALF else (db, eb)
        lanes = slice(at, at + BLOCK)
        total = own_rows(i, mp)[:, lanes].astype(F32)
        total = total + direct[i % HALF, :, lanes].astype(F32) + summed[i % HALF, :, lanes].astype(F32)
        ob[b] = jnp.where(token < fills[b], total, 0.0).astype(BF16)
    for j in range(N_DP):
        first = jnp.int32(0)
        second = jnp.int32(0)
        for b in range(blocks - 1, -1, -1):
            here = ranks[b] == j
            second = jnp.where(here, first, second)
            first = jnp.where(here, b, first)
        a2s[0, j] = ob[first]
        a2s[1, j] = ob[second]
    start_slots(0, 0)
    start_slots(0, 1)
    for k in range(CAP):
        pltpu.make_async_copy(a2s.at[k, dp], a2o.at[k, dp], lsem.at[k]).start()
    proj_up = big_end(0)
    qdh[...] = stack2(proj_up)

    def fresh_up(i, carry):
        small_add(1, fold2(mm(qdh[...], xall[i])), gp[i])
        return carry


    lax.fori_loop(0, NC, fresh_up, 0)
    scatter(3, small[1])
    start_slots(0, 2)
    start_slots(0, 3)
    y_start(1, 2, collect(2))
    elim[0] = identity_at_right((RANK, 2 * RANK))
    elim[0, :, :RANK] = gram_of(proj_up)
    arrived(gbuf.at[pl.ds(0, N_MP - 1)], xr.at[1])
    gram_d = gbuf[0]
    for j in range(1, N_MP):
        gram_d = gram_d + gbuf[j]
    elim[1] = identity_at_right((RANK, 2 * RANK))
    elim[1, : RANK // 2, :RANK] = gram_d[:, :RANK]
    elim[1, RANK // 2 :, :RANK] = gram_d[:, RANK:]
    elim[...] = eliminate(elim[...], 0, 8)
    spread(2, y_end(1, 2))
    start_slots(1, 0)
    elim[...] = eliminate(elim[...], 8, 24)
    spread(3, collect(3))
    start_slots(1, 1)
    start_slots(1, 2)
    start_slots(1, 3)
    elim[...] = eliminate(elim[...], 24, RANK - 1)
    inv_u = left4(inverse_of_factor(elim[0]).T)
    inv_d = left4(inverse_of_factor(elim[1]).T)
    f4u[...] = left4(mm_tn(inv_u, right4(proj_up))).T
    f4d[...] = left4(mm_tn(inv_d, right4(proj_down))).T
    pltpu.make_async_copy(f4u, a4u, lsem.at[2]).start()
    pltpu.make_async_copy(f4d, a4d, lsem.at[3]).start()
    arrived(erb.at[pl.ds(0, N_DP - 1)], xr.at[0])
    for r in range(N_DP):
        era_out[r : r + 1, :] = erb[r, 0:1, :]
    big_start(1, 2)
    out_landed(0)
    new_u = mm_tn(inv_u, right4(small_end(1, 3)))
    qnu[...] = new_u
    new_d = mm_tn(inv_d, right4(big_end(1)))
    qnd[...] = new_d
    out_landed(1)

    pltpu.make_async_copy(f4u, a4u, lsem.at[2]).wait()
    pltpu.make_async_copy(f4d, a4d, lsem.at[3]).wait()
    left_here(xall.at[:, pl.ds(0, 7 * feats), :], gsem.at[0])
    left_here(call.at[:, pl.ds(0, 7 * feats), :], gsem.at[1])
    left_here(po, ossem.at[0])
    left_here(erb.at[pl.ds(0, N_DP - 1)], xs.at[0])
    left_here(gbuf.at[pl.ds(0, N_MP - 1)], xs.at[1])
    for group, ref in enumerate((ra, rb, ea, eb, da, db)):
        left_here(ref, yssem.at[group])
    for ph in range(2):
        left_here(pbuf.at[ph], mrs.at[ph, 0])
        left_here(bigf.at[ph, 0], mrs.at[ph, 1])
        left_here(ybuf.at[ph, pl.ds(0, N_Y - 1)], ars.at[2 * ph, 2])
    for q in range(4):
        left_here(rcv.at[q, pl.ds(0, N_DP - 1)], ars.at[q, 0])
        left_here(agb.at[q, pl.ds(0, N_DP - 1)], ars.at[q, 1])
    for k in range(CAP):
        left_here(a2s.at[k, pl.ds(0, N_DP - 1)], a2ss.at[k])
        pltpu.make_async_copy(a2s.at[k, dp], a2o.at[k, dp], lsem.at[k]).wait()


def layer_kernel(ranks, fills, pt, ct, wu, wd, qu, qd):
    feats, tokens = pt.shape
    tc = tokens // NC
    width, ff = wu.shape
    half = width // 2
    vm = pl.BlockSpec(memory_space=pltpu.VMEM)
    sm = pl.BlockSpec(memory_space=pltpu.SMEM)
    anywhere = pl.BlockSpec(memory_space=pl.ANY)
    shape = jax.ShapeDtypeStruct
    outs = [
        shape((CAP, N_DP, feats, BLOCK), BF16),
        shape((width, 4 * RANK), BF16),
        shape((ff, 4 * RANK), BF16),
        shape((N_DP, 128), jnp.int32),
        shape((RANK, ff), F32),
        shape((RANK, width), F32),
    ]
    dma = pltpu.SemaphoreType.DMA
    scratch = [
        pltpu.VMEM((NC, width, tc), BF16),
        pltpu.VMEM((NC, width, tc), BF16),
        pltpu.VMEM((NC, ff, tc), BF16),
        pltpu.VMEM((NC, ff, tc), BF16),
        pltpu.VMEM((width, ff), BF16),
        pltpu.VMEM((ff, width), BF16),
        pltpu.VMEM((RANK, ff), F32),
        pltpu.VMEM((RANK, width), F32),
        pltpu.VMEM((ff, width), BF16),
        pltpu.VMEM((width, ff), BF16),
        pltpu.VMEM((2 * RANK, ff), BF16),
        pltpu.VMEM((2 * RANK, width), BF16),
        pltpu.VMEM((2, 2, RANK, half), F32),
        pltpu.VMEM((2, RANK, ff), F32),
        pltpu.VMEM((2, RANK, half), F32),
        pltpu.VMEM((4, N_DP, 4, half), F32),
        pltpu.VMEM((4, N_DP, 4, half), F32),
        pltpu.VMEM((2, 4, half), F32),
        pltpu.VMEM((2, N_Y, 4, half), F32),
        pltpu.VMEM((4, N_DP, 4, half), F32),
        pltpu.VMEM((2, 2, RANK, half), F32),
        pltpu.VMEM((2, RANK, 2 * RANK), F32),
        pltpu.VMEM((N_MP, RANK // 2, 2 * RANK), F32),
        pltpu.VMEM((NC, 2, N_Y * feats, tc), BF16),
        pltpu.VMEM((NC, N_Y * feats, tc), BF16),
        pltpu.VMEM((NC, N_Y * feats, tc), BF16),
    ]
    scratch += [pltpu.VMEM((HALF, feats, tc), BF16) for _ in range(8)]
    scratch += [
        pltpu.VMEM((tokens // BLOCK, feats, BLOCK), BF16),
        pltpu.VMEM((CAP, N_DP, feats, BLOCK), BF16),
        pltpu.VMEM((width, 4 * RANK), BF16),
        pltpu.VMEM((ff, 4 * RANK), BF16),
        pltpu.VMEM((8, 128), jnp.int32),
        pltpu.VMEM((N_DP, 8, 128), jnp.int32),
        dma((6,)),
        dma((NC, 3)),
        dma((NC,)),
        dma((2,)),
        dma((NC,)),
        dma((1,)),
        dma((6,)),
        dma((6,)),
        dma((4, 3)),
        dma((4, 3)),
        dma((2, 2)),
        dma((2, 2)),
        dma((2,)),
        dma((2,)),
        dma((CAP,)),
        dma((CAP,)),
    ]
    return pl.pallas_call(
        kernel_body,
        out_shape=outs,
        in_specs=[sm] * 2 + [anywhere] * 6,
        out_specs=[anywhere] * 3 + [vm] * 3,
        scratch_shapes=scratch,
        compiler_params=pltpu.CompilerParams(
            collective_id=0, has_side_effects=True, vmem_limit_bytes=60 * 1024 * 1024
        ),
        name="layer",
    )(ranks, fills, pt, ct, wu, wd, qu, qd)


def finish_body(
    ranks, landed, a4u, a4d, qnu, qnd,
    enc, up, down, new_u, new_d,
    blocks, placed, ups, downs, b4u, b4d, origin, sems,
):
    me = lax.axis_index("dp")
    for k in range(CAP):
        pltpu.make_async_copy(landed.at[k], blocks.at[pl.ds(k * N_DP, N_DP)], sems.at[10 + k]).start()
    copies = []
    b4u[...] = right4(qnu[...])
    b4d[...] = right4(qnd[...])
    for k, (a, b, stage, out) in enumerate(((a4u, b4u, ups, up), (a4d, b4d, downs, down))):
        pieces = 2
        size = stage.shape[0] // pieces
        for j in range(pieces):
            at = pl.ds(j * size, size)
            stage[at, :] = mm(a[at, :], b[...])
            copy = pltpu.make_async_copy(stage.at[at, :], out.at[at, :], sems.at[k * pieces + j])
            copy.start()
            copies.append(copy)
    new_u[...] = qnu[...]
    new_d[...] = qnd[...]
    for slot in range(RMAX + 1):
        origin[slot] = CAP * N_DP
    filled = jnp.int32(0)
    for r in range(N_DP):
        seen = jnp.int32(0)
        for b in range(BLK_DEV):
            hit = (ranks[r, b] == me).astype(jnp.int32)
            held = origin[filled]
            origin[filled] = jnp.where(hit > 0, seen * N_DP + r, held)
            seen = seen + hit
            filled = filled + hit
    blocks[CAP * N_DP] = jnp.zeros_like(blocks[CAP * N_DP])
    for k in range(CAP):
        pltpu.make_async_copy(landed.at[k], blocks.at[pl.ds(k * N_DP, N_DP)], sems.at[10 + k]).wait()
    for slot in range(RMAX):
        placed[:, slot * BLOCK : (slot + 1) * BLOCK] = blocks[origin[slot]]
    copy = pltpu.make_async_copy(placed, enc, sems.at[12])
    copy.start()
    copies.append(copy)
    for copy in copies:
        copy.wait()


def finish(landed, a4u, a4d, ranks, qnu, qnd):
    feats = landed.shape[2]
    width, ff = a4u.shape[0], a4d.shape[0]
    vm = pl.BlockSpec(memory_space=pltpu.VMEM)
    anywhere = pl.BlockSpec(memory_space=pl.ANY)
    shape = jax.ShapeDtypeStruct
    return pl.pallas_call(
        finish_body,
        out_shape=[
            shape((feats, RMAX * BLOCK), BF16),
            shape((width, ff), F32),
            shape((ff, width), F32),
            shape(qnu.shape, F32),
            shape(qnd.shape, F32),
        ],
        in_specs=[pl.BlockSpec(memory_space=pltpu.SMEM), anywhere] + [vm] * 4,
        out_specs=[anywhere] * 3 + [vm] * 2,
        scratch_shapes=[
            pltpu.VMEM((CAP * N_DP + 1, *landed.shape[2:]), BF16),
            pltpu.VMEM((feats, RMAX * BLOCK), BF16),
            pltpu.VMEM((width, ff), F32),
            pltpu.VMEM((ff, width), F32),
            pltpu.VMEM((4 * RANK, ff), BF16),
            pltpu.VMEM((4 * RANK, width), BF16),
            pltpu.SMEM((RMAX + 1,), jnp.int32),
            pltpu.SemaphoreType.DMA((13,)),
        ],
        name="finish",
    )(ranks, landed, a4u, a4d, qnu, qnd)


def local(patches, cotangent, encoder_rank, block_fill, w_up, w_down, q_up, q_down):
    results = layer_kernel(
        encoder_rank, block_fill, patches.T, cotangent.T, w_up, w_down, q_up.T, q_down.T
    )
    encoded, approx_up, approx_down, new_u, new_d = finish(*results)
    return (encoded.T, approx_up, approx_down, new_u.T, new_d.T)


def solution(mesh):
    in_specs = (
        P("dp", "mp"), P("dp", "mp"), P("dp"), P("dp"), P(None, "mp"), P("mp", None), P("mp", None), P(),
    )
    out_specs = (P("dp", "mp"), P(None, "mp"), P("mp", None), P("mp", None), P())
    return jax.shard_map(local, mesh=mesh, in_specs=in_specs, out_specs=out_specs, check_vma=False)
```

```python
import jax
import jax.numpy as jnp
from jax import lax
from jax.experimental import pallas as pl
from jax.experimental.pallas import tpu as pltpu
from jax.sharding import PartitionSpec as P

BLOCK = 128
CAP = 2
RMAX = 18
BLK_DEV = 12
N_DP = 16
N_Y = 4
N_MP = 8
GROUPS = ((1, 4, 10, 15), (2, 8, 7, 13), (3, 12, 5, 11), (6, 9, 14))
RANK = 64
NC = 6
HALF = NC // 2
AHEAD = 2
MESH = pl.DeviceIdType.MESH
F32 = jnp.float32
BF16 = jnp.bfloat16
NT = (((1,), (1,)), ((), ()))
TN = (((0,), (0,)), ((), ()))


def mm(a, b):
    return jnp.dot(a, b, preferred_element_type=F32)


def mm_nt(a, b):
    return lax.dot_general(a, b, NT, preferred_element_type=F32)


def mm_tn(a, b):
    return lax.dot_general(a, b, TN, preferred_element_type=F32)


def parts(v):
    hi = v.astype(BF16)
    lo = (v - hi.astype(F32)).astype(BF16)
    return hi, lo


def stack2(v):
    return jnp.concatenate(parts(v), axis=0)


def fold2(v):
    return v[:RANK] + v[RANK:]


def left4(v):
    hi, lo = parts(v)
    return jnp.concatenate([hi, hi, lo, lo], axis=0)


def right4(v):
    hi, lo = parts(v)
    return jnp.concatenate([hi, lo, hi, lo], axis=0)


def gram_of(v):
    s = stack2(v)
    g = mm_nt(s, s)
    return g[:RANK, :RANK] + g[:RANK, RANK:] + g[RANK:, :RANK] + g[RANK:, RANK:]


def eliminate(w, first, last):
    row = lax.broadcasted_iota(jnp.int32, w.shape, 1)
    for k in range(first, last):
        pivot = w[:, k : k + 1, k : k + 1]
        line = w[:, k : k + 1, :] * (1.0 / pivot)
        w = w - jnp.where(row > k, w[:, :, k : k + 1] * line, 0.0)
    return w


def identity_at_right(shape):
    row = lax.broadcasted_iota(jnp.int32, shape, 0)
    lane = lax.broadcasted_iota(jnp.int32, shape, 1)
    return jnp.where(lane == row + RANK, 1.0, 0.0).astype(F32)


def inverse_of_factor(w):
    row = lax.broadcasted_iota(jnp.int32, w.shape, 0)
    lane = lax.broadcasted_iota(jnp.int32, w.shape, 1)
    diag = jnp.sum(jnp.where(lane == row, w, 0.0), axis=1, keepdims=True)
    return (w * lax.rsqrt(diag))[:, RANK:]


def kernel_body(
    ranks, fills, pt, ct, wu, wd, qu, qd,
    a2o, a4u, a4d, era_out, qnu, qnd,
    xall, call, hid, gp, wus, wds, qus, qds, wut, wdt, quh, qdh,
    proj, small, pbuf, rsb, rcv, ysend, ybuf, agb, bigf, elim,
    gbuf, outp, po, osb, ra, rb, da, db, fa, fb, ea, eb, ob, a2s, f4u, f4d, ers, erb,
    lsem, nsem, msem, gsem, osem, ossem, ysem, yssem, arr, ars, mrr, mrs, xr, xs, a2rr, a2ss,
):
    dp = lax.axis_index("dp")
    mp = lax.axis_index("mp")
    y = mp // 2
    c = mp % 2
    right = ((y + 1) % N_Y) * 2 + c
    left = ((y + 3) % N_Y) * 2 + c
    far = ((y + 2) % N_Y) * 2 + c
    mate = y * 2 + (1 - c)
    feats = pt.shape[0]
    tc = xall.shape[2]
    per = tc // BLOCK
    blocks = NC * per
    half = proj.shape[3]

    def send(src, dst, ssem, rsem, dpi, mpi):
        return pltpu.make_async_remote_copy(
            src_ref=src, dst_ref=dst, send_sem=ssem, recv_sem=rsem,
            device_id=(dpi, mpi), device_id_type=MESH,
        )

    def arrived(ref, sem):
        send(ref, ref, sem, sem, dp, mate).wait_recv()

    def left_here(ref, sem):
        send(ref, ref, sem, sem, dp, mate).wait_send()

    def fetched(ref, sem):
        pltpu.make_async_copy(ref, ref, sem).wait()

    def dp_at(t):
        return ((dp // N_Y + t // N_Y) % N_Y) * N_Y + (dp + t) % N_Y

    def mp_at(t):
        return (mp + t) % N_MP

    def rows(ref, i, owner):
        return ref.at[i, pl.ds(pl.multiple_of(owner * feats, 32), feats), :]

    barrier = pltpu.get_barrier_semaphore()
    for t in range(1, N_DP):
        pl.semaphore_signal(barrier, inc=1, device_id=(dp_at(t), mp), device_id_type=MESH)
    for t in range(1, N_MP):
        pl.semaphore_signal(barrier, inc=1, device_id=(dp, mp_at(t)), device_id_type=MESH)

    def fetch(src, dst, i, sem):
        pltpu.make_async_copy(src.at[:, pl.ds(i * tc, tc)], rows(dst, i, mp), lsem.at[sem]).start()

    for i in range(NC):
        fetch(ct, call, i, 0 if i < AHEAD else 6)
        fetch(pt, xall, i, 1 if i < AHEAD else 7)
    weights = ((wu, wus), (wd, wds), (qu, qus), (qd, qds))
    for k, (src, dst) in enumerate(weights):
        pltpu.make_async_copy(src, dst, lsem.at[2 + k]).start()
    token = lax.broadcasted_iota(jnp.int32, (feats, BLOCK), 1)
    def mask_cot(i):
        place_at = pl.ds(pl.multiple_of(mp * feats, 32), feats)
        for k in range(per):
            lanes = slice(k * BLOCK, (k + 1) * BLOCK)
            kept = jnp.where(token < fills[i * per + k], call[i, place_at, lanes].astype(F32), 0.0)
            call[i, place_at, lanes] = kept.astype(BF16)

    fetched(call.at[0, pl.ds(0, AHEAD * feats), :], lsem.at[0])
    for i in range(AHEAD):
        mask_cot(i)
    fetched(xall.at[0, pl.ds(0, AHEAD * feats), :], lsem.at[1])
    pl.semaphore_wait(barrier, N_DP + N_MP - 2)

    def pass_on(ref, which, i, owner, to, rsem):
        send(rows(ref, i, owner), rows(ref, i, owner), gsem.at[which], rsem, dp, to).start()

    def start_own(i):
        pass_on(xall, 0, i, mp, right, nsem.at[i, 0])
        pass_on(call, 1, i, mp, left, nsem.at[i, 0])
        pass_on(call, 1, i, mp, right, nsem.at[i, 1])
        pass_on(xall, 0, i, mp, left, nsem.at[i, 1])

    def pair(i):
        return xall.at[i, pl.ds(0, 2 * feats), :]

    for i in range(AHEAD):
        start_own(i)
    fetched(call.at[0, pl.ds(0, (NC - AHEAD) * feats), :], lsem.at[6])
    fetched(xall.at[0, pl.ds(0, (NC - AHEAD) * feats), :], lsem.at[7])
    for i in range(AHEAD, NC):
        mask_cot(i)
    for i in range(NC):
        pass_on(xall, 0, i, mp, mate, msem.at[i])
        pass_on(call, 1, i, mp, mate, msem.at[i])
    lane8 = lax.broadcasted_iota(jnp.int32, (8, 128), 1)
    mine = jnp.zeros((8, 128), jnp.int32)
    for b in range(blocks):
        mine = jnp.where(lane8 == b, ranks[b], mine)
    ers[...] = mine
    erb[dp] = mine
    for t in range(1, N_DP):
        send(ers, erb.at[dp], xs.at[0], xr.at[0], dp_at(t), mp).start()

    for k, (src, dst) in enumerate(weights):
        fetched(dst, lsem.at[2 + k])
    for j in range(wus.shape[1] // 128):
        wut[j * 128 : (j + 1) * 128, :] = wus[:, j * 128 : (j + 1) * 128].T
    for j in range(wds.shape[1] // 128):
        wdt[j * 128 : (j + 1) * 128, :] = wds[:, j * 128 : (j + 1) * 128].T
    quh[...] = stack2(qus[...])
    qdh[...] = stack2(qds[...])
    for ph in range(2):
        proj[ph] = jnp.zeros_like(proj[ph])
        small[ph] = jnp.zeros_like(small[ph])

    def start_out(i):
        send(outp.at[i, 1 - c], po.at[i], ossem.at[0], osem.at[i], dp, mate).start()

    def out_sum(i):
        arrived(po.at[i], osem.at[i])
        osb[i] = (outp[i, c].astype(F32) + po[i].astype(F32)).astype(BF16)

    def work_a(i):
        pre = mm(wut[...], xall[i])
        grad = mm(wds[...], call[i])
        sig = jax.nn.sigmoid(1.702 * pre)
        act = pre * sig
        hid[i] = act.astype(BF16)
        gp[i] = (grad * (sig + 1.702 * act * (1.0 - sig))).astype(BF16)

    def work_b(i):
        o = mm(wdt[...], hid[i]).astype(BF16)
        for m in range(N_MP):
            at = (m // 2) * feats
            outp[i, m % 2, at : at + feats, :] = o[m * feats : (m + 1) * feats]
        start_out(i)

    def big_add(ph, rows64, other):
        big = fold2(mm_nt(stack2(rows64), other))
        proj[ph, 0] += big[:, :half]
        proj[ph, 1] += big[:, half:]

    def small_add(ph, rows64, other):
        small[ph] += fold2(mm_nt(stack2(rows64), other))

    def add_projection(i):
        big_add(0, fold2(mm(quh[...], gp[i])), xall[i])
        small_add(0, fold2(mm(qdh[...], call[i])), hid[i])

    def piece(first, owner):
        at = pl.multiple_of((owner // 2) * feats, 32)
        return osb.at[pl.ds(first, HALF), pl.ds(at, feats), :]

    def own_rows(i, owner):
        return osb[i, pl.ds(pl.multiple_of((owner // 2) * feats, 32), feats), :]

    def send_a(j):
        y_send(osb.at[j, pl.ds(pl.multiple_of((right // 2) * feats, 32), feats), :], da.at[j], 4, right)

    def send_b(i):
        j = i - HALF
        y_send(osb.at[i, pl.ds(pl.multiple_of((far // 2) * feats, 32), feats), :], rb.at[j], 1, right)
        y_send(osb.at[i, pl.ds(pl.multiple_of((left // 2) * feats, 32), feats), :], db.at[j], 5, left)

    def y_send(src, dst, group, to):
        send(src, dst, yssem.at[group], ysem.at[group], dp, to).start()

    def mate_start(ph):
        send(proj.at[ph, 1 - c], pbuf.at[ph], mrs.at[ph, 0], mrr.at[ph, 0], dp, mate).start()

    def mate_end(ph):
        arrived(pbuf.at[ph], mrr.at[ph, 0])
        return proj[ph, c] + pbuf[ph]

    def scatter(q, value):
        for j in range(N_DP):
            rsb[q, j] = value[4 * j : 4 * j + 4]
        for t in range(1, N_DP):
            to = dp_at(t)
            send(rsb.at[q, to], rcv.at[q, dp], ars.at[q, 0], arr.at[q, 0], to, mp).start()
        rcv[q, dp] = rsb[q, dp]

    def collect(q):
        arrived(rcv.at[q, pl.ds(0, N_DP - 1)], arr.at[q, 0])
        total = rcv[q, 0]
        for j in range(1, N_DP):
            total = total + rcv[q, j]
        return total

    def y_start(ph, q, total):
        ysend[ph] = total
        for t in range(1, N_Y):
            to = ((y + t) % N_Y) * 2 + c
            send(ysend.at[ph], ybuf.at[ph, y], ars.at[q, 2], arr.at[q, 2], dp, to).start()
        ybuf[ph, y] = total

    def y_end(ph, q):
        arrived(ybuf.at[ph, pl.ds(0, N_Y - 1)], arr.at[q, 2])
        total = ybuf[ph, 0]
        for j in range(1, N_Y):
            total = total + ybuf[ph, j]
        return total

    def spread(q, total):
        agb[q, dp] = total
        for t in range(1, N_DP):
            send(agb.at[q, dp], agb.at[q, dp], ars.at[q, 1], arr.at[q, 1], dp_at(t), mp).start()

    def small_end(ph, q):
        arrived(agb.at[q, pl.ds(0, N_DP - 1)], arr.at[q, 1])
        for j in range(N_DP):
            small[ph, 4 * j : 4 * j + 4] = agb[q, j]
        return small[ph]

    def big_start(ph, q):
        arrived(agb.at[q, pl.ds(0, N_DP - 1)], arr.at[q, 1])
        for j in range(N_DP):
            bigf[ph, c, 4 * j : 4 * j + 4] = agb[q, j]
        send(bigf.at[ph, c], bigf.at[ph, c], mrs.at[ph, 1], mrr.at[ph, 1], dp, mate).start()

    def big_end(ph):
        arrived(bigf.at[ph, 0], mrr.at[ph, 1])
        return jnp.concatenate([bigf[ph, 0], bigf[ph, 1]], axis=1)

    def step(i, carry):
        @pl.when(i < NC)
        def _():
            arrived(pair(i), nsem.at[i, 0])
            pass_on(xall, 0, i, left, right, nsem.at[i, 2])
            pass_on(call, 1, i, right, left, nsem.at[i, 2])

            @pl.when(i + AHEAD < NC)
            def _():
                start_own(i + AHEAD)

            pass_on(xall, 0, i, left, mate, msem.at[i])
            pass_on(call, 1, i, right, mate, msem.at[i])

        @pl.when(jnp.logical_and(i > 1, i < NC + 2))
        def _():
            arrived(xall.at[i - 2], msem.at[i - 2])
            work_a(i - 2)

        @pl.when(i < NC)
        def _():
            arrived(pair(i), nsem.at[i, 1])
            pass_on(call, 1, i, left, mate, msem.at[i])
            pass_on(xall, 0, i, right, mate, msem.at[i])

        @pl.when(jnp.logical_and(i > 1, i < NC + 2))
        def _():
            add_projection(i - 2)

        @pl.when(jnp.logical_and(i > 2, i <= NC))
        def _():
            out_sum(i - 3)

        @pl.when(i == NC)
        def _():
            y_send(piece(0, far), ra, 0, left)
            send_b(HALF)
            for j in range(HALF - 1):
                send_a(j)

        @pl.when(jnp.logical_and(i > 0, i <= NC))
        def _():
            arrived(pair(i - 1), nsem.at[i - 1, 2])
            pass_on(xall, 0, i - 1, far, mate, msem.at[i - 1])
            pass_on(call, 1, i - 1, far, mate, msem.at[i - 1])

        @pl.when(i == NC + 3)
        def _():
            scatter(0, mate_end(0))

        @pl.when(jnp.logical_or(jnp.logical_and(i > 1, i < NC), i > NC + 1))
        def _():
            work_b(jnp.where(i < NC, i - 2, i - 4))

        @pl.when(i == NC + 1)
        def _():
            mate_start(0)
            scatter(1, small[0])

        return carry

    lax.fori_loop(0, NC + 4, step, 0)

    def start_slots(k, group):
        for t in GROUPS[group]:
            to = dp_at(t)
            send(a2s.at[k, to], a2o.at[k, dp], a2ss.at[k], a2rr.at[k], to, mp).start()

    def out_landed(k):
        arrived(a2o.at[k, pl.ds(0, N_DP - 1)], a2rr.at[k])

    for i in range(HALF + 1, NC):
        out_sum(i)
        send_b(i)
    send_a(HALF - 1)
    arrived(ra, ysem.at[0])
    for i in range(HALF):
        fa[i] = (own_rows(i, left).astype(F32) + ra[i].astype(F32)).astype(BF16)
    spread(1, collect(1))
    y_start(0, 0, collect(0))
    y_send(fa, ea, 2, left)
    arrived(rb, ysem.at[1])
    for i in range(HALF):
        fb[i] = (own_rows(HALF + i, right).astype(F32) + rb[i].astype(F32)).astype(BF16)
    y_send(fb, eb, 3, right)
    spread(0, y_end(0, 0))
    proj_down = small_end(0, 1)
    quh[:, :half] = stack2(proj_down)

    def fresh_down(i, carry):
        big_add(1, fold2(mm(quh[...], hid[i])), call[i])
        return carry

    lax.fori_loop(0, NC, fresh_down, 0, unroll=2)
    mate_start(1)
    gram_d = gram_of(proj_down)
    gbuf[mp] = jnp.concatenate([gram_d[: RANK // 2], gram_d[RANK // 2 :]], axis=1)
    for t in range(1, N_MP):
        send(gbuf.at[mp], gbuf.at[mp], xs.at[1], xr.at[1], dp, mp_at(t)).start()
    big_start(0, 0)
    scatter(2, mate_end(1))
    arrived(ea, ysem.at[2])
    arrived(eb, ysem.at[3])
    arrived(da, ysem.at[4])
    arrived(db, ysem.at[5])
    for b in range(blocks):
        i, at = b // per, (b % per) * BLOCK
        direct, summed = (da, ea) if i < HALF else (db, eb)
        lanes = slice(at, at + BLOCK)
        total = own_rows(i, mp)[:, lanes].astype(F32)
        total = total + direct[i % HALF, :, lanes].astype(F32) + summed[i % HALF, :, lanes].astype(F32)
        ob[b] = jnp.where(token < fills[b], total, 0.0).astype(BF16)
    for j in range(N_DP):
        first = jnp.int32(0)
        second = jnp.int32(0)
        for b in range(blocks - 1, -1, -1):
            here = ranks[b] == j
            second = jnp.where(here, first, second)
            first = jnp.where(here, b, first)
        a2s[0, j] = ob[first]
        a2s[1, j] = ob[second]
    start_slots(0, 0)
    start_slots(0, 1)
    for k in range(CAP):
        pltpu.make_async_copy(a2s.at[k, dp], a2o.at[k, dp], lsem.at[k]).start()
    proj_up = big_end(0)
    qdh[...] = stack2(proj_up)

    def fresh_up(i, carry):
        small_add(1, fold2(mm(qdh[...], xall[i])), gp[i])
        return carry


    lax.fori_loop(0, NC, fresh_up, 0, unroll=2)
    scatter(3, small[1])
    start_slots(0, 2)
    start_slots(0, 3)
    y_start(1, 2, collect(2))
    elim[0] = identity_at_right((RANK, 2 * RANK))
    elim[0, :, :RANK] = gram_of(proj_up)
    arrived(gbuf.at[pl.ds(0, N_MP - 1)], xr.at[1])
    gram_d = gbuf[0]
    for j in range(1, N_MP):
        gram_d = gram_d + gbuf[j]
    elim[1] = identity_at_right((RANK, 2 * RANK))
    elim[1, : RANK // 2, :RANK] = gram_d[:, :RANK]
    elim[1, RANK // 2 :, :RANK] = gram_d[:, RANK:]
    elim[...] = eliminate(elim[...], 0, 8)
    spread(2, y_end(1, 2))
    start_slots(1, 0)
    elim[...] = eliminate(elim[...], 8, 24)
    spread(3, collect(3))
    start_slots(1, 1)
    start_slots(1, 2)
    start_slots(1, 3)
    elim[...] = eliminate(elim[...], 24, RANK - 1)
    inv_u = left4(inverse_of_factor(elim[0]).T)
    inv_d = left4(inverse_of_factor(elim[1]).T)
    f4u[...] = left4(mm_tn(inv_u, right4(proj_up))).T
    f4d[...] = left4(mm_tn(inv_d, right4(proj_down))).T
    pltpu.make_async_copy(f4u, a4u, lsem.at[2]).start()
    pltpu.make_async_copy(f4d, a4d, lsem.at[3]).start()
    arrived(erb.at[pl.ds(0, N_DP - 1)], xr.at[0])
    for r in range(N_DP):
        era_out[r : r + 1, :] = erb[r, 0:1, :]
    big_start(1, 2)
    out_landed(0)
    new_u = mm_tn(inv_u, right4(small_end(1, 3)))
    qnu[...] = new_u
    new_d = mm_tn(inv_d, right4(big_end(1)))
    qnd[...] = new_d
    out_landed(1)

    pltpu.make_async_copy(f4u, a4u, lsem.at[2]).wait()
    pltpu.make_async_copy(f4d, a4d, lsem.at[3]).wait()
    left_here(xall.at[:, pl.ds(0, 7 * feats), :], gsem.at[0])
    left_here(call.at[:, pl.ds(0, 7 * feats), :], gsem.at[1])
    left_here(po, ossem.at[0])
    left_here(erb.at[pl.ds(0, N_DP - 1)], xs.at[0])
    left_here(gbuf.at[pl.ds(0, N_MP - 1)], xs.at[1])
    for group, ref in enumerate((ra, rb, ea, eb, da, db)):
        left_here(ref, yssem.at[group])
    for ph in range(2):
        left_here(pbuf.at[ph], mrs.at[ph, 0])
        left_here(bigf.at[ph, 0], mrs.at[ph, 1])
        left_here(ybuf.at[ph, pl.ds(0, N_Y - 1)], ars.at[2 * ph, 2])
    for q in range(4):
        left_here(rcv.at[q, pl.ds(0, N_DP - 1)], ars.at[q, 0])
        left_here(agb.at[q, pl.ds(0, N_DP - 1)], ars.at[q, 1])
    for k in range(CAP):
        left_here(a2s.at[k, pl.ds(0, N_DP - 1)], a2ss.at[k])
        pltpu.make_async_copy(a2s.at[k, dp], a2o.at[k, dp], lsem.at[k]).wait()


def layer_kernel(ranks, fills, pt, ct, wu, wd, qu, qd):
    feats, tokens = pt.shape
    tc = tokens // NC
    width, ff = wu.shape
    half = width // 2
    vm = pl.BlockSpec(memory_space=pltpu.VMEM)
    sm = pl.BlockSpec(memory_space=pltpu.SMEM)
    anywhere = pl.BlockSpec(memory_space=pl.ANY)
    shape = jax.ShapeDtypeStruct
    outs = [
        shape((CAP, N_DP, feats, BLOCK), BF16),
        shape((width, 4 * RANK), BF16),
        shape((ff, 4 * RANK), BF16),
        shape((N_DP, 128), jnp.int32),
        shape((RANK, ff), F32),
        shape((RANK, width), F32),
    ]
    dma = pltpu.SemaphoreType.DMA
    scratch = [
        pltpu.VMEM((NC, width, tc), BF16),
        pltpu.VMEM((NC, width, tc), BF16),
        pltpu.VMEM((NC, ff, tc), BF16),
        pltpu.VMEM((NC, ff, tc), BF16),
        pltpu.VMEM((width, ff), BF16),
        pltpu.VMEM((ff, width), BF16),
        pltpu.VMEM((RANK, ff), F32),
        pltpu.VMEM((RANK, width), F32),
        pltpu.VMEM((ff, width), BF16),
        pltpu.VMEM((width, ff), BF16),
        pltpu.VMEM((2 * RANK, ff), BF16),
        pltpu.VMEM((2 * RANK, width), BF16),
        pltpu.VMEM((2, 2, RANK, half), F32),
        pltpu.VMEM((2, RANK, ff), F32),
        pltpu.VMEM((2, RANK, half), F32),
        pltpu.VMEM((4, N_DP, 4, half), F32),
        pltpu.VMEM((4, N_DP, 4, half), F32),
        pltpu.VMEM((2, 4, half), F32),
        pltpu.VMEM((2, N_Y, 4, half), F32),
        pltpu.VMEM((4, N_DP, 4, half), F32),
        pltpu.VMEM((2, 2, RANK, half), F32),
        pltpu.VMEM((2, RANK, 2 * RANK), F32),
        pltpu.VMEM((N_MP, RANK // 2, 2 * RANK), F32),
        pltpu.VMEM((NC, 2, N_Y * feats, tc), BF16),
        pltpu.VMEM((NC, N_Y * feats, tc), BF16),
        pltpu.VMEM((NC, N_Y * feats, tc), BF16),
    ]
    scratch += [pltpu.VMEM((HALF, feats, tc), BF16) for _ in range(8)]
    scratch += [
        pltpu.VMEM((tokens // BLOCK, feats, BLOCK), BF16),
        pltpu.VMEM((CAP, N_DP, feats, BLOCK), BF16),
        pltpu.VMEM((width, 4 * RANK), BF16),
        pltpu.VMEM((ff, 4 * RANK), BF16),
        pltpu.VMEM((8, 128), jnp.int32),
        pltpu.VMEM((N_DP, 8, 128), jnp.int32),
        dma((8,)),
        dma((NC, 3)),
        dma((NC,)),
        dma((2,)),
        dma((NC,)),
        dma((1,)),
        dma((6,)),
        dma((6,)),
        dma((4, 3)),
        dma((4, 3)),
        dma((2, 2)),
        dma((2, 2)),
        dma((2,)),
        dma((2,)),
        dma((CAP,)),
        dma((CAP,)),
    ]
    return pl.pallas_call(
        kernel_body,
        out_shape=outs,
        in_specs=[sm] * 2 + [anywhere] * 6,
        out_specs=[anywhere] * 3 + [vm] * 3,
        scratch_shapes=scratch,
        compiler_params=pltpu.CompilerParams(
            collective_id=0, has_side_effects=True, vmem_limit_bytes=60 * 1024 * 1024
        ),
        name="layer",
    )(ranks, fills, pt, ct, wu, wd, qu, qd)


def finish_body(
    ranks, landed, a4u, a4d, qnu, qnd,
    enc, up, down, new_u, new_d,
    blocks, placed, ups, downs, b4u, b4d, origin, sems,
):
    me = lax.axis_index("dp")
    for k in range(CAP):
        pltpu.make_async_copy(landed.at[k], blocks.at[pl.ds(k * N_DP, N_DP)], sems.at[10 + k]).start()
    copies = []
    b4u[...] = right4(qnu[...])
    b4d[...] = right4(qnd[...])
    for k, (a, b, stage, out) in enumerate(((a4u, b4u, ups, up), (a4d, b4d, downs, down))):
        pieces = 2
        size = stage.shape[0] // pieces
        for j in range(pieces):
            at = pl.ds(j * size, size)
            stage[at, :] = mm(a[at, :], b[...])
            copy = pltpu.make_async_copy(stage.at[at, :], out.at[at, :], sems.at[k * pieces + j])
            copy.start()
            copies.append(copy)
    new_u[...] = qnu[...]
    new_d[...] = qnd[...]
    for slot in range(RMAX + 1):
        origin[slot] = CAP * N_DP
    filled = jnp.int32(0)
    for r in range(N_DP):
        seen = jnp.int32(0)
        for b in range(BLK_DEV):
            hit = (ranks[r, b] == me).astype(jnp.int32)
            held = origin[filled]
            origin[filled] = jnp.where(hit > 0, seen * N_DP + r, held)
            seen = seen + hit
            filled = filled + hit
    blocks[CAP * N_DP] = jnp.zeros_like(blocks[CAP * N_DP])
    for k in range(CAP):
        pltpu.make_async_copy(landed.at[k], blocks.at[pl.ds(k * N_DP, N_DP)], sems.at[10 + k]).wait()
    for slot in range(RMAX):
        placed[:, slot * BLOCK : (slot + 1) * BLOCK] = blocks[origin[slot]]
    copy = pltpu.make_async_copy(placed, enc, sems.at[12])
    copy.start()
    copies.append(copy)
    for copy in copies:
        copy.wait()


def finish(landed, a4u, a4d, ranks, qnu, qnd):
    feats = landed.shape[2]
    width, ff = a4u.shape[0], a4d.shape[0]
    vm = pl.BlockSpec(memory_space=pltpu.VMEM)
    anywhere = pl.BlockSpec(memory_space=pl.ANY)
    shape = jax.ShapeDtypeStruct
    return pl.pallas_call(
        finish_body,
        out_shape=[
            shape((feats, RMAX * BLOCK), BF16),
            shape((width, ff), F32),
            shape((ff, width), F32),
            shape(qnu.shape, F32),
            shape(qnd.shape, F32),
        ],
        in_specs=[pl.BlockSpec(memory_space=pltpu.SMEM), anywhere] + [vm] * 4,
        out_specs=[anywhere] * 3 + [vm] * 2,
        scratch_shapes=[
            pltpu.VMEM((CAP * N_DP + 1, *landed.shape[2:]), BF16),
            pltpu.VMEM((feats, RMAX * BLOCK), BF16),
            pltpu.VMEM((width, ff), F32),
            pltpu.VMEM((ff, width), F32),
            pltpu.VMEM((4 * RANK, ff), BF16),
            pltpu.VMEM((4 * RANK, width), BF16),
            pltpu.SMEM((RMAX + 1,), jnp.int32),
            pltpu.SemaphoreType.DMA((13,)),
        ],
        name="finish",
    )(ranks, landed, a4u, a4d, qnu, qnd)


def local(patches, cotangent, encoder_rank, block_fill, w_up, w_down, q_up, q_down):
    results = layer_kernel(
        encoder_rank, block_fill, patches.T, cotangent.T, w_up, w_down, q_up.T, q_down.T
    )
    encoded, approx_up, approx_down, new_u, new_d = finish(*results)
    return (encoded.T, approx_up, approx_down, new_u.T, new_d.T)


def solution(mesh):
    in_specs = (
        P("dp", "mp"), P("dp", "mp"), P("dp"), P("dp"), P(None, "mp"), P("mp", None), P("mp", None), P(),
    )
    out_specs = (P("dp", "mp"), P(None, "mp"), P("mp", None), P("mp", None), P())
    return jax.shard_map(local, mesh=mesh, in_specs=in_specs, out_specs=out_specs, check_vma=False)
```

```python
import jax
import jax.numpy as jnp
from jax import lax
from jax.experimental import pallas as pl
from jax.experimental.pallas import tpu as pltpu
from jax.sharding import PartitionSpec as P

BLOCK = 128
CAP = 2
RMAX = 18
BLK_DEV = 12
N_DP = 16
N_Y = 4
N_MP = 8
GROUPS = ((1, 4, 10, 15), (2, 8, 7, 13), (3, 12, 5, 11), (6, 9, 14))
RANK = 64
NC = 6
HALF = NC // 2
AHEAD = 2
MESH = pl.DeviceIdType.MESH
F32 = jnp.float32
BF16 = jnp.bfloat16
NT = (((1,), (1,)), ((), ()))
TN = (((0,), (0,)), ((), ()))


def mm(a, b):
    return jnp.dot(a, b, preferred_element_type=F32)


def mm_nt(a, b):
    return lax.dot_general(a, b, NT, preferred_element_type=F32)


def mm_tn(a, b):
    return lax.dot_general(a, b, TN, preferred_element_type=F32)


def parts(v):
    hi = v.astype(BF16)
    lo = (v - hi.astype(F32)).astype(BF16)
    return hi, lo


def stack2(v):
    return jnp.concatenate(parts(v), axis=0)


def fold2(v):
    return v[:RANK] + v[RANK:]


def left4(v):
    hi, lo = parts(v)
    return jnp.concatenate([hi, hi, lo, lo], axis=0)


def right4(v):
    hi, lo = parts(v)
    return jnp.concatenate([hi, lo, hi, lo], axis=0)


def gram_of(v):
    s = stack2(v)
    g = mm_nt(s, s)
    return g[:RANK, :RANK] + g[:RANK, RANK:] + g[RANK:, :RANK] + g[RANK:, RANK:]


def eliminate(w, first, last):
    row = lax.broadcasted_iota(jnp.int32, w.shape, 1)
    for k in range(first, last):
        pivot = w[:, k : k + 1, k : k + 1]
        line = w[:, k : k + 1, :] * (1.0 / pivot)
        w = w - jnp.where(row > k, w[:, :, k : k + 1] * line, 0.0)
    return w


def identity_at_right(shape):
    row = lax.broadcasted_iota(jnp.int32, shape, 0)
    lane = lax.broadcasted_iota(jnp.int32, shape, 1)
    return jnp.where(lane == row + RANK, 1.0, 0.0).astype(F32)


def inverse_of_factor(w):
    row = lax.broadcasted_iota(jnp.int32, w.shape, 0)
    lane = lax.broadcasted_iota(jnp.int32, w.shape, 1)
    diag = jnp.sum(jnp.where(lane == row, w, 0.0), axis=1, keepdims=True)
    return (w * lax.rsqrt(diag))[:, RANK:]


def kernel_body(
    ranks, fills, pt, ct, wu, wd, qu, qd,
    a2o, a4u, a4d, era_out, qnu, qnd,
    xall, call, hid, gp, wus, wds, qus, qds, wut, wdt, quh, qdh,
    proj, small, pbuf, rsb, rcv, ysend, ybuf, agb, bigf, elim,
    gbuf, outp, po, osb, ra, rb, da, db, fa, fb, ea, eb, ob, a2s, f4u, f4d, fu, fd, ef, ers, erb,
    lsem, nsem, msem, gsem, osem, ossem, ysem, yssem, arr, ars, mrr, mrs, xr, xs, a2rr, a2ss,
):
    dp = lax.axis_index("dp")
    mp = lax.axis_index("mp")
    y = mp // 2
    c = mp % 2
    right = ((y + 1) % N_Y) * 2 + c
    left = ((y + 3) % N_Y) * 2 + c
    far = ((y + 2) % N_Y) * 2 + c
    mate = y * 2 + (1 - c)
    feats = pt.shape[0]
    tc = xall.shape[2]
    per = tc // BLOCK
    blocks = NC * per
    half = proj.shape[3]

    def send(src, dst, ssem, rsem, dpi, mpi):
        return pltpu.make_async_remote_copy(
            src_ref=src, dst_ref=dst, send_sem=ssem, recv_sem=rsem,
            device_id=(dpi, mpi), device_id_type=MESH,
        )

    def arrived(ref, sem):
        send(ref, ref, sem, sem, dp, mate).wait_recv()

    def left_here(ref, sem):
        send(ref, ref, sem, sem, dp, mate).wait_send()

    def fetched(ref, sem):
        pltpu.make_async_copy(ref, ref, sem).wait()

    def dp_at(t):
        return ((dp // N_Y + t // N_Y) % N_Y) * N_Y + (dp + t) % N_Y

    def mp_at(t):
        return (mp + t) % N_MP

    def rows(ref, i, owner):
        return ref.at[i, pl.ds(pl.multiple_of(owner * feats, 32), feats), :]

    barrier = pltpu.get_barrier_semaphore()
    for t in range(1, N_DP):
        pl.semaphore_signal(barrier, inc=1, device_id=(dp_at(t), mp), device_id_type=MESH)
    for t in range(1, N_MP):
        pl.semaphore_signal(barrier, inc=1, device_id=(dp, mp_at(t)), device_id_type=MESH)

    def fetch(src, dst, i, sem):
        pltpu.make_async_copy(src.at[:, pl.ds(i * tc, tc)], rows(dst, i, mp), lsem.at[sem]).start()

    for i in range(NC):
        fetch(ct, call, i, 0 if i < AHEAD else 6)
        fetch(pt, xall, i, 1 if i < AHEAD else 7)
    weights = ((wu, wus), (wd, wds), (qu, qus), (qd, qds))
    for k, (src, dst) in enumerate(weights):
        pltpu.make_async_copy(src, dst, lsem.at[2 + k]).start()
    token = lax.broadcasted_iota(jnp.int32, (feats, BLOCK), 1)
    def mask_cot(i):
        place_at = pl.ds(pl.multiple_of(mp * feats, 32), feats)
        for k in range(per):
            lanes = slice(k * BLOCK, (k + 1) * BLOCK)
            kept = jnp.where(token < fills[i * per + k], call[i, place_at, lanes].astype(F32), 0.0)
            call[i, place_at, lanes] = kept.astype(BF16)

    fetched(call.at[0, pl.ds(0, AHEAD * feats), :], lsem.at[0])
    for i in range(AHEAD):
        mask_cot(i)
    fetched(xall.at[0, pl.ds(0, AHEAD * feats), :], lsem.at[1])
    pl.semaphore_wait(barrier, N_DP + N_MP - 2)

    def pass_on(ref, which, i, owner, to, rsem):
        send(rows(ref, i, owner), rows(ref, i, owner), gsem.at[which], rsem, dp, to).start()

    def start_own(i):
        pass_on(xall, 0, i, mp, right, nsem.at[i, 0])
        pass_on(call, 1, i, mp, left, nsem.at[i, 0])
        pass_on(call, 1, i, mp, right, nsem.at[i, 1])
        pass_on(xall, 0, i, mp, left, nsem.at[i, 1])

    def pair(i):
        return xall.at[i, pl.ds(0, 2 * feats), :]

    for i in range(AHEAD):
        start_own(i)
    fetched(call.at[0, pl.ds(0, (NC - AHEAD) * feats), :], lsem.at[6])
    fetched(xall.at[0, pl.ds(0, (NC - AHEAD) * feats), :], lsem.at[7])
    for i in range(AHEAD, NC):
        mask_cot(i)
    for i in range(NC):
        pass_on(xall, 0, i, mp, mate, msem.at[i])
        pass_on(call, 1, i, mp, mate, msem.at[i])
    lane8 = lax.broadcasted_iota(jnp.int32, (8, 128), 1)
    mine = jnp.zeros((8, 128), jnp.int32)
    for b in range(blocks):
        mine = jnp.where(lane8 == b, ranks[b], mine)
    ers[...] = mine
    erb[dp] = mine
    for t in range(1, N_DP):
        send(ers, erb.at[dp], xs.at[0], xr.at[0], dp_at(t), mp).start()

    for k, (src, dst) in enumerate(weights):
        fetched(dst, lsem.at[2 + k])
    for j in range(wus.shape[1] // 128):
        wut[j * 128 : (j + 1) * 128, :] = wus[:, j * 128 : (j + 1) * 128].T
    for j in range(wds.shape[1] // 128):
        wdt[j * 128 : (j + 1) * 128, :] = wds[:, j * 128 : (j + 1) * 128].T
    quh[...] = stack2(qus[...])
    qdh[...] = stack2(qds[...])
    for ph in range(2):
        proj[ph] = jnp.zeros_like(proj[ph])
        small[ph] = jnp.zeros_like(small[ph])

    def start_out(i):
        send(outp.at[i, 1 - c], po.at[i], ossem.at[0], osem.at[i], dp, mate).start()

    def out_sum(i):
        arrived(po.at[i], osem.at[i])
        osb[i] = (outp[i, c].astype(F32) + po[i].astype(F32)).astype(BF16)

    def work_a(i):
        pre = mm(wut[...], xall[i])
        grad = mm(wds[...], call[i])
        sig = jax.nn.sigmoid(1.702 * pre)
        act = pre * sig
        hid[i] = act.astype(BF16)
        gp[i] = (grad * (sig + 1.702 * act * (1.0 - sig))).astype(BF16)

    def work_b(i):
        o = mm(wdt[...], hid[i]).astype(BF16)
        for m in range(N_MP):
            at = (m // 2) * feats
            outp[i, m % 2, at : at + feats, :] = o[m * feats : (m + 1) * feats]
        start_out(i)

    def big_add(ph, rows64, other):
        big = fold2(mm_nt(stack2(rows64), other))
        proj[ph, 0] += big[:, :half]
        proj[ph, 1] += big[:, half:]

    def small_add(ph, rows64, other):
        small[ph] += fold2(mm_nt(stack2(rows64), other))

    def add_projection(i):
        big_add(0, fold2(mm(quh[...], gp[i])), xall[i])
        small_add(0, fold2(mm(qdh[...], call[i])), hid[i])

    def piece(first, owner):
        at = pl.multiple_of((owner // 2) * feats, 32)
        return osb.at[pl.ds(first, HALF), pl.ds(at, feats), :]

    def own_rows(i, owner):
        return osb[i, pl.ds(pl.multiple_of((owner // 2) * feats, 32), feats), :]

    def send_a(j):
        y_send(osb.at[j, pl.ds(pl.multiple_of((right // 2) * feats, 32), feats), :], da.at[j], 4, right)

    def send_b(i):
        j = i - HALF
        y_send(osb.at[i, pl.ds(pl.multiple_of((far // 2) * feats, 32), feats), :], rb.at[j], 1, right)
        y_send(osb.at[i, pl.ds(pl.multiple_of((left // 2) * feats, 32), feats), :], db.at[j], 5, left)

    def y_send(src, dst, group, to):
        send(src, dst, yssem.at[group], ysem.at[group], dp, to).start()

    def mate_start(ph):
        send(proj.at[ph, 1 - c], pbuf.at[ph], mrs.at[ph, 0], mrr.at[ph, 0], dp, mate).start()

    def mate_end(ph):
        arrived(pbuf.at[ph], mrr.at[ph, 0])
        return proj[ph, c] + pbuf[ph]

    def scatter(q, value):
        for j in range(N_DP):
            rsb[q, j] = value[4 * j : 4 * j + 4]
        for t in range(1, N_DP):
            to = dp_at(t)
            send(rsb.at[q, to], rcv.at[q, dp], ars.at[q, 0], arr.at[q, 0], to, mp).start()
        rcv[q, dp] = rsb[q, dp]

    def collect(q):
        arrived(rcv.at[q, pl.ds(0, N_DP - 1)], arr.at[q, 0])
        total = rcv[q, 0]
        for j in range(1, N_DP):
            total = total + rcv[q, j]
        return total

    def y_start(ph, q, total):
        ysend[ph] = total
        for t in range(1, N_Y):
            to = ((y + t) % N_Y) * 2 + c
            send(ysend.at[ph], ybuf.at[ph, y], ars.at[q, 2], arr.at[q, 2], dp, to).start()
        ybuf[ph, y] = total

    def y_end(ph, q):
        arrived(ybuf.at[ph, pl.ds(0, N_Y - 1)], arr.at[q, 2])
        total = ybuf[ph, 0]
        for j in range(1, N_Y):
            total = total + ybuf[ph, j]
        return total

    def spread(q, total):
        agb[q, dp] = total
        for t in range(1, N_DP):
            send(agb.at[q, dp], agb.at[q, dp], ars.at[q, 1], arr.at[q, 1], dp_at(t), mp).start()

    def small_end(ph, q):
        arrived(agb.at[q, pl.ds(0, N_DP - 1)], arr.at[q, 1])
        for j in range(N_DP):
            small[ph, 4 * j : 4 * j + 4] = agb[q, j]
        return small[ph]

    def big_start(ph, q):
        arrived(agb.at[q, pl.ds(0, N_DP - 1)], arr.at[q, 1])
        for j in range(N_DP):
            bigf[ph, c, 4 * j : 4 * j + 4] = agb[q, j]
        send(bigf.at[ph, c], bigf.at[ph, c], mrs.at[ph, 1], mrr.at[ph, 1], dp, mate).start()

    def big_end(ph):
        arrived(bigf.at[ph, 0], mrr.at[ph, 1])
        return jnp.concatenate([bigf[ph, 0], bigf[ph, 1]], axis=1)

    def step(i, carry):
        @pl.when(i < NC)
        def _():
            arrived(pair(i), nsem.at[i, 0])
            pass_on(xall, 0, i, left, right, nsem.at[i, 2])
            pass_on(call, 1, i, right, left, nsem.at[i, 2])

            @pl.when(i + AHEAD < NC)
            def _():
                start_own(i + AHEAD)

            pass_on(xall, 0, i, left, mate, msem.at[i])
            pass_on(call, 1, i, right, mate, msem.at[i])

        @pl.when(jnp.logical_and(i > 1, i < NC + 2))
        def _():
            arrived(xall.at[i - 2], msem.at[i - 2])
            work_a(i - 2)

        @pl.when(i < NC)
        def _():
            arrived(pair(i), nsem.at[i, 1])
            pass_on(call, 1, i, left, mate, msem.at[i])
            pass_on(xall, 0, i, right, mate, msem.at[i])

        @pl.when(jnp.logical_and(i > 1, i < NC + 2))
        def _():
            add_projection(i - 2)

        @pl.when(jnp.logical_and(i > 2, i <= NC))
        def _():
            out_sum(i - 3)

        @pl.when(i == NC)
        def _():
            y_send(piece(0, far), ra, 0, left)
            send_b(HALF)
            for j in range(HALF - 1):
                send_a(j)

        @pl.when(jnp.logical_and(i > 0, i <= NC))
        def _():
            arrived(pair(i - 1), nsem.at[i - 1, 2])
            pass_on(xall, 0, i - 1, far, mate, msem.at[i - 1])
            pass_on(call, 1, i - 1, far, mate, msem.at[i - 1])

        @pl.when(i == NC + 3)
        def _():
            scatter(0, mate_end(0))

        @pl.when(jnp.logical_or(jnp.logical_and(i > 1, i < NC), i > NC + 1))
        def _():
            work_b(jnp.where(i < NC, i - 2, i - 4))

        @pl.when(i == NC + 1)
        def _():
            mate_start(0)
            scatter(1, small[0])

        return carry

    lax.fori_loop(0, NC + 4, step, 0)

    def start_slots(k, group):
        for t in GROUPS[group]:
            to = dp_at(t)
            send(a2s.at[k, to], a2o.at[k, dp], a2ss.at[k], a2rr.at[k], to, mp).start()

    def out_landed(k):
        arrived(a2o.at[k, pl.ds(0, N_DP - 1)], a2rr.at[k])

    for i in range(HALF + 1, NC):
        out_sum(i)
        send_b(i)
    send_a(HALF - 1)
    arrived(ra, ysem.at[0])
    for i in range(HALF):
        fa[i] = (own_rows(i, left).astype(F32) + ra[i].astype(F32)).astype(BF16)
    spread(1, collect(1))
    y_start(0, 0, collect(0))
    y_send(fa, ea, 2, left)
    arrived(rb, ysem.at[1])
    for i in range(HALF):
        fb[i] = (own_rows(HALF + i, right).astype(F32) + rb[i].astype(F32)).astype(BF16)
    y_send(fb, eb, 3, right)
    spread(0, y_end(0, 0))
    proj_down = small_end(0, 1)
    quh[:, :half] = stack2(proj_down)

    def fresh_down(i, carry):
        big_add(1, fold2(mm(quh[...], hid[i])), call[i])
        return carry

    lax.fori_loop(0, NC, fresh_down, 0, unroll=2)
    mate_start(1)
    gram_d = gram_of(proj_down)
    gbuf[mp] = jnp.concatenate([gram_d[: RANK // 2], gram_d[RANK // 2 :]], axis=1)
    for t in range(1, N_MP):
        send(gbuf.at[mp], gbuf.at[mp], xs.at[1], xr.at[1], dp, mp_at(t)).start()
    big_start(0, 0)
    scatter(2, mate_end(1))
    arrived(ea, ysem.at[2])
    arrived(eb, ysem.at[3])
    arrived(da, ysem.at[4])
    arrived(db, ysem.at[5])
    for b in range(blocks):
        i, at = b // per, (b % per) * BLOCK
        direct, summed = (da, ea) if i < HALF else (db, eb)
        lanes = slice(at, at + BLOCK)
        total = own_rows(i, mp)[:, lanes].astype(F32)
        total = total + direct[i % HALF, :, lanes].astype(F32) + summed[i % HALF, :, lanes].astype(F32)
        ob[b] = jnp.where(token < fills[b], total, 0.0).astype(BF16)
    for j in range(N_DP):
        first = jnp.int32(0)
        second = jnp.int32(0)
        for b in range(blocks - 1, -1, -1):
            here = ranks[b] == j
            second = jnp.where(here, first, second)
            first = jnp.where(here, b, first)
        a2s[0, j] = ob[first]
        a2s[1, j] = ob[second]
    start_slots(0, 0)
    start_slots(0, 1)
    for k in range(CAP):
        pltpu.make_async_copy(a2s.at[k, dp], a2o.at[k, dp], lsem.at[k]).start()
    proj_up = big_end(0)
    qdh[...] = stack2(proj_up)

    def fresh_up(i, carry):
        small_add(1, fold2(mm(qdh[...], xall[i])), gp[i])
        return carry


    lax.fori_loop(0, NC, fresh_up, 0, unroll=2)
    scatter(3, small[1])
    start_slots(0, 2)
    start_slots(0, 3)
    y_start(1, 2, collect(2))
    elim[0] = identity_at_right((RANK, 2 * RANK))
    elim[0, :, :RANK] = gram_of(proj_up)
    arrived(gbuf.at[pl.ds(0, N_MP - 1)], xr.at[1])
    gram_d = gbuf[0]
    for j in range(1, N_MP):
        gram_d = gram_d + gbuf[j]
    elim[1] = identity_at_right((RANK, 2 * RANK))
    elim[1, : RANK // 2, :RANK] = gram_d[:, :RANK]
    elim[1, RANK // 2 :, :RANK] = gram_d[:, RANK:]
    start_slots(1, 0)
    elim[...] = eliminate(elim[...], 0, 8)
    spread(2, y_end(1, 2))
    start_slots(1, 1)
    elim[...] = eliminate(elim[...], 8, 24)
    spread(3, collect(3))
    start_slots(1, 2)
    start_slots(1, 3)
    elim[...] = eliminate(elim[...], 24, RANK - 1)
    inv_u = left4(inverse_of_factor(elim[0]).T)
    inv_d = left4(inverse_of_factor(elim[1]).T)
    f4u[...] = left4(mm_tn(inv_u, right4(proj_up))).T
    f4d[...] = left4(mm_tn(inv_d, right4(proj_down))).T
    pltpu.make_async_copy(f4u, a4u, lsem.at[2]).start()
    pltpu.make_async_copy(f4d, a4d, lsem.at[3]).start()
    arrived(erb.at[pl.ds(0, N_DP - 1)], xr.at[0])
    for r in range(N_DP):
        ef[r : r + 1, :] = erb[r, 0:1, :]
    pltpu.make_async_copy(ef, era_out, lsem.at[4]).start()
    big_start(1, 2)
    out_landed(0)
    new_u = mm_tn(inv_u, right4(small_end(1, 3)))
    fu[...] = new_u
    pltpu.make_async_copy(fu, qnu, lsem.at[5]).start()
    new_d = mm_tn(inv_d, right4(big_end(1)))
    fd[...] = new_d
    pltpu.make_async_copy(fd, qnd, lsem.at[6]).start()
    out_landed(1)

    pltpu.make_async_copy(f4u, a4u, lsem.at[2]).wait()
    pltpu.make_async_copy(f4d, a4d, lsem.at[3]).wait()
    pltpu.make_async_copy(ef, era_out, lsem.at[4]).wait()
    pltpu.make_async_copy(fu, qnu, lsem.at[5]).wait()
    pltpu.make_async_copy(fd, qnd, lsem.at[6]).wait()
    left_here(xall.at[:, pl.ds(0, 7 * feats), :], gsem.at[0])
    left_here(call.at[:, pl.ds(0, 7 * feats), :], gsem.at[1])
    left_here(po, ossem.at[0])
    left_here(erb.at[pl.ds(0, N_DP - 1)], xs.at[0])
    left_here(gbuf.at[pl.ds(0, N_MP - 1)], xs.at[1])
    for group, ref in enumerate((ra, rb, ea, eb, da, db)):
        left_here(ref, yssem.at[group])
    for ph in range(2):
        left_here(pbuf.at[ph], mrs.at[ph, 0])
        left_here(bigf.at[ph, 0], mrs.at[ph, 1])
        left_here(ybuf.at[ph, pl.ds(0, N_Y - 1)], ars.at[2 * ph, 2])
    for q in range(4):
        left_here(rcv.at[q, pl.ds(0, N_DP - 1)], ars.at[q, 0])
        left_here(agb.at[q, pl.ds(0, N_DP - 1)], ars.at[q, 1])
    for k in range(CAP):
        left_here(a2s.at[k, pl.ds(0, N_DP - 1)], a2ss.at[k])
        pltpu.make_async_copy(a2s.at[k, dp], a2o.at[k, dp], lsem.at[k]).wait()


def layer_kernel(ranks, fills, pt, ct, wu, wd, qu, qd):
    feats, tokens = pt.shape
    tc = tokens // NC
    width, ff = wu.shape
    half = width // 2
    sm = pl.BlockSpec(memory_space=pltpu.SMEM)
    anywhere = pl.BlockSpec(memory_space=pl.ANY)
    shape = jax.ShapeDtypeStruct
    outs = [
        shape((CAP, N_DP, feats, BLOCK), BF16),
        shape((width, 4 * RANK), BF16),
        shape((ff, 4 * RANK), BF16),
        shape((N_DP, 128), jnp.int32),
        shape((RANK, ff), F32),
        shape((RANK, width), F32),
    ]
    dma = pltpu.SemaphoreType.DMA
    scratch = [
        pltpu.VMEM((NC, width, tc), BF16),
        pltpu.VMEM((NC, width, tc), BF16),
        pltpu.VMEM((NC, ff, tc), BF16),
        pltpu.VMEM((NC, ff, tc), BF16),
        pltpu.VMEM((width, ff), BF16),
        pltpu.VMEM((ff, width), BF16),
        pltpu.VMEM((RANK, ff), F32),
        pltpu.VMEM((RANK, width), F32),
        pltpu.VMEM((ff, width), BF16),
        pltpu.VMEM((width, ff), BF16),
        pltpu.VMEM((2 * RANK, ff), BF16),
        pltpu.VMEM((2 * RANK, width), BF16),
        pltpu.VMEM((2, 2, RANK, half), F32),
        pltpu.VMEM((2, RANK, ff), F32),
        pltpu.VMEM((2, RANK, half), F32),
        pltpu.VMEM((4, N_DP, 4, half), F32),
        pltpu.VMEM((4, N_DP, 4, half), F32),
        pltpu.VMEM((2, 4, half), F32),
        pltpu.VMEM((2, N_Y, 4, half), F32),
        pltpu.VMEM((4, N_DP, 4, half), F32),
        pltpu.VMEM((2, 2, RANK, half), F32),
        pltpu.VMEM((2, RANK, 2 * RANK), F32),
        pltpu.VMEM((N_MP, RANK // 2, 2 * RANK), F32),
        pltpu.VMEM((NC, 2, N_Y * feats, tc), BF16),
        pltpu.VMEM((NC, N_Y * feats, tc), BF16),
        pltpu.VMEM((NC, N_Y * feats, tc), BF16),
    ]
    scratch += [pltpu.VMEM((HALF, feats, tc), BF16) for _ in range(8)]
    scratch += [
        pltpu.VMEM((tokens // BLOCK, feats, BLOCK), BF16),
        pltpu.VMEM((CAP, N_DP, feats, BLOCK), BF16),
        pltpu.VMEM((width, 4 * RANK), BF16),
        pltpu.VMEM((ff, 4 * RANK), BF16),
        pltpu.VMEM((RANK, ff), F32),
        pltpu.VMEM((RANK, width), F32),
        pltpu.VMEM((N_DP, 128), jnp.int32),
        pltpu.VMEM((8, 128), jnp.int32),
        pltpu.VMEM((N_DP, 8, 128), jnp.int32),
        dma((8,)),
        dma((NC, 3)),
        dma((NC,)),
        dma((2,)),
        dma((NC,)),
        dma((1,)),
        dma((6,)),
        dma((6,)),
        dma((4, 3)),
        dma((4, 3)),
        dma((2, 2)),
        dma((2, 2)),
        dma((2,)),
        dma((2,)),
        dma((CAP,)),
        dma((CAP,)),
    ]
    return pl.pallas_call(
        kernel_body,
        out_shape=outs,
        in_specs=[sm] * 2 + [anywhere] * 6,
        out_specs=[anywhere] * len(outs),
        scratch_shapes=scratch,
        compiler_params=pltpu.CompilerParams(
            collective_id=0, has_side_effects=True, vmem_limit_bytes=60 * 1024 * 1024
        ),
        name="layer",
    )(ranks, fills, pt, ct, wu, wd, qu, qd)


def finish_body(
    ranks, landed, a4u, a4d, qnu, qnd,
    enc, up, down, new_u, new_d,
    blocks, placed, ups, downs, b4u, b4d, origin, sems,
):
    me = lax.axis_index("dp")
    for k in range(CAP):
        pltpu.make_async_copy(landed.at[k], blocks.at[pl.ds(k * N_DP, N_DP)], sems.at[10 + k]).start()
    copies = []
    b4u[...] = right4(qnu[...])
    b4d[...] = right4(qnd[...])
    for k, (a, b, stage, out) in enumerate(((a4u, b4u, ups, up), (a4d, b4d, downs, down))):
        pieces = 2
        size = stage.shape[0] // pieces
        for j in range(pieces):
            at = pl.ds(j * size, size)
            stage[at, :] = mm(a[at, :], b[...])
            copy = pltpu.make_async_copy(stage.at[at, :], out.at[at, :], sems.at[k * pieces + j])
            copy.start()
            copies.append(copy)
    new_u[...] = qnu[...]
    new_d[...] = qnd[...]
    for slot in range(RMAX + 1):
        origin[slot] = CAP * N_DP
    filled = jnp.int32(0)
    for r in range(N_DP):
        seen = jnp.int32(0)
        for b in range(BLK_DEV):
            hit = (ranks[r, b] == me).astype(jnp.int32)
            held = origin[filled]
            origin[filled] = jnp.where(hit > 0, seen * N_DP + r, held)
            seen = seen + hit
            filled = filled + hit
    blocks[CAP * N_DP] = jnp.zeros_like(blocks[CAP * N_DP])
    for k in range(CAP):
        pltpu.make_async_copy(landed.at[k], blocks.at[pl.ds(k * N_DP, N_DP)], sems.at[10 + k]).wait()
    for slot in range(RMAX):
        placed[:, slot * BLOCK : (slot + 1) * BLOCK] = blocks[origin[slot]]
    copy = pltpu.make_async_copy(placed, enc, sems.at[12])
    copy.start()
    copies.append(copy)
    for copy in copies:
        copy.wait()


def finish(landed, a4u, a4d, ranks, qnu, qnd):
    feats = landed.shape[2]
    width, ff = a4u.shape[0], a4d.shape[0]
    vm = pl.BlockSpec(memory_space=pltpu.VMEM)
    anywhere = pl.BlockSpec(memory_space=pl.ANY)
    shape = jax.ShapeDtypeStruct
    return pl.pallas_call(
        finish_body,
        out_shape=[
            shape((feats, RMAX * BLOCK), BF16),
            shape((width, ff), F32),
            shape((ff, width), F32),
            shape(qnu.shape, F32),
            shape(qnd.shape, F32),
        ],
        in_specs=[pl.BlockSpec(memory_space=pltpu.SMEM), anywhere] + [vm] * 4,
        out_specs=[anywhere] * 3 + [vm] * 2,
        scratch_shapes=[
            pltpu.VMEM((CAP * N_DP + 1, *landed.shape[2:]), BF16),
            pltpu.VMEM((feats, RMAX * BLOCK), BF16),
            pltpu.VMEM((width, ff), F32),
            pltpu.VMEM((ff, width), F32),
            pltpu.VMEM((4 * RANK, ff), BF16),
            pltpu.VMEM((4 * RANK, width), BF16),
            pltpu.SMEM((RMAX + 1,), jnp.int32),
            pltpu.SemaphoreType.DMA((13,)),
        ],
        name="finish",
    )(ranks, landed, a4u, a4d, qnu, qnd)


def local(patches, cotangent, encoder_rank, block_fill, w_up, w_down, q_up, q_down):
    results = layer_kernel(
        encoder_rank, block_fill, patches.T, cotangent.T, w_up, w_down, q_up.T, q_down.T
    )
    encoded, approx_up, approx_down, new_u, new_d = finish(*results)
    return (encoded.T, approx_up, approx_down, new_u.T, new_d.T)


def solution(mesh):
    in_specs = (
        P("dp", "mp"), P("dp", "mp"), P("dp"), P("dp"), P(None, "mp"), P("mp", None), P("mp", None), P(),
    )
    out_specs = (P("dp", "mp"), P(None, "mp"), P("mp", None), P("mp", None), P())
    return jax.shard_map(local, mesh=mesh, in_specs=in_specs, out_specs=out_specs, check_vma=False)
```

```python
import jax
import jax.numpy as jnp
from jax import lax
from jax.experimental import pallas as pl
from jax.experimental.pallas import tpu as pltpu
from jax.sharding import PartitionSpec as P

BLOCK = 128
CAP = 2
RMAX = 18
BLK_DEV = 12
N_DP = 16
N_Y = 4
N_MP = 8
GROUPS = ((1, 4, 10, 15), (2, 8, 7, 13), (3, 12, 5, 11), (6, 9, 14))
RANK = 64
NC = 6
HALF = NC // 2
AHEAD = 2
MESH = pl.DeviceIdType.MESH
F32 = jnp.float32
BF16 = jnp.bfloat16
NT = (((1,), (1,)), ((), ()))
TN = (((0,), (0,)), ((), ()))


def mm(a, b):
    return jnp.dot(a, b, preferred_element_type=F32)


def mm_nt(a, b):
    return lax.dot_general(a, b, NT, preferred_element_type=F32)


def mm_tn(a, b):
    return lax.dot_general(a, b, TN, preferred_element_type=F32)


def parts(v):
    hi = v.astype(BF16)
    lo = (v - hi.astype(F32)).astype(BF16)
    return hi, lo


def stack2(v):
    return jnp.concatenate(parts(v), axis=0)


def fold2(v):
    return v[:RANK] + v[RANK:]


def left4(v):
    hi, lo = parts(v)
    return jnp.concatenate([hi, hi, lo, lo], axis=0)


def right4(v):
    hi, lo = parts(v)
    return jnp.concatenate([hi, lo, hi, lo], axis=0)


def gram_of(v):
    s = stack2(v)
    g = mm_nt(s, s)
    return g[:RANK, :RANK] + g[:RANK, RANK:] + g[RANK:, :RANK] + g[RANK:, RANK:]


def eliminate(w, first, last):
    row = lax.broadcasted_iota(jnp.int32, w.shape, 1)
    for k in range(first, last):
        pivot = w[:, k : k + 1, k : k + 1]
        line = w[:, k : k + 1, :] * (1.0 / pivot)
        w = w - jnp.where(row > k, w[:, :, k : k + 1] * line, 0.0)
    return w


def identity_at_right(shape):
    row = lax.broadcasted_iota(jnp.int32, shape, 0)
    lane = lax.broadcasted_iota(jnp.int32, shape, 1)
    return jnp.where(lane == row + RANK, 1.0, 0.0).astype(F32)


def inverse_of_factor(w):
    row = lax.broadcasted_iota(jnp.int32, w.shape, 0)
    lane = lax.broadcasted_iota(jnp.int32, w.shape, 1)
    diag = jnp.sum(jnp.where(lane == row, w, 0.0), axis=1, keepdims=True)
    return (w * lax.rsqrt(diag))[:, RANK:]


def kernel_body(
    ranks, fills, pt, ct, wu, wd, qu, qd,
    a2o, a4u, a4d, era_out, qnu, qnd,
    xall, call, hid, gp, wus, wds, qus, qds, wut, wdt, quh, qdh,
    proj, small, pbuf, rsb, rcv, ysend, ybuf, agb, bigf, elim,
    gbuf, outp, po, osb, ra, rb, da, db, fa, fb, ea, eb, ob, a2s, f4u, f4d, fu, fd, ef, ers, erb,
    lsem, nsem, msem, gsem, osem, ossem, ysem, yssem, arr, ars, mrr, mrs, xr, xs, a2rr, a2ss,
):
    dp = lax.axis_index("dp")
    mp = lax.axis_index("mp")
    y = mp // 2
    c = mp % 2
    right = ((y + 1) % N_Y) * 2 + c
    left = ((y + 3) % N_Y) * 2 + c
    far = ((y + 2) % N_Y) * 2 + c
    mate = y * 2 + (1 - c)
    feats = pt.shape[0]
    tc = xall.shape[2]
    per = tc // BLOCK
    blocks = NC * per
    half = proj.shape[3]

    def send(src, dst, ssem, rsem, dpi, mpi):
        return pltpu.make_async_remote_copy(
            src_ref=src, dst_ref=dst, send_sem=ssem, recv_sem=rsem,
            device_id=(dpi, mpi), device_id_type=MESH,
        )

    def arrived(ref, sem):
        send(ref, ref, sem, sem, dp, mate).wait_recv()

    def left_here(ref, sem):
        send(ref, ref, sem, sem, dp, mate).wait_send()

    def fetched(ref, sem):
        pltpu.make_async_copy(ref, ref, sem).wait()

    def dp_at(t):
        return ((dp // N_Y + t // N_Y) % N_Y) * N_Y + (dp + t) % N_Y

    def mp_at(t):
        return (mp + t) % N_MP

    def rows(ref, i, owner):
        return ref.at[i, pl.ds(pl.multiple_of(owner * feats, 32), feats), :]

    barrier = pltpu.get_barrier_semaphore()
    for t in range(1, N_DP):
        pl.semaphore_signal(barrier, inc=1, device_id=(dp_at(t), mp), device_id_type=MESH)
    for t in range(1, N_MP):
        pl.semaphore_signal(barrier, inc=1, device_id=(dp, mp_at(t)), device_id_type=MESH)

    def fetch(src, dst, i, sem):
        pltpu.make_async_copy(src.at[:, pl.ds(i * tc, tc)], rows(dst, i, mp), lsem.at[sem]).start()

    for i in range(NC):
        fetch(ct, call, i, 0 if i < AHEAD else 6)
        fetch(pt, xall, i, 1 if i < AHEAD else 7)
    weights = ((wu, wus), (wd, wds), (qu, qus), (qd, qds))
    for k, (src, dst) in enumerate(weights):
        pltpu.make_async_copy(src, dst, lsem.at[2 + k]).start()
    token = lax.broadcasted_iota(jnp.int32, (feats, BLOCK), 1)
    def mask_cot(i):
        place_at = pl.ds(pl.multiple_of(mp * feats, 32), feats)
        for k in range(per):
            lanes = slice(k * BLOCK, (k + 1) * BLOCK)
            kept = jnp.where(token < fills[i * per + k], call[i, place_at, lanes].astype(F32), 0.0)
            call[i, place_at, lanes] = kept.astype(BF16)

    fetched(call.at[0, pl.ds(0, AHEAD * feats), :], lsem.at[0])
    for i in range(AHEAD):
        mask_cot(i)
    fetched(xall.at[0, pl.ds(0, AHEAD * feats), :], lsem.at[1])
    pl.semaphore_wait(barrier, N_DP + N_MP - 2)

    def pass_on(ref, which, i, owner, to, rsem):
        send(rows(ref, i, owner), rows(ref, i, owner), gsem.at[which], rsem, dp, to).start()

    def start_own(i):
        pass_on(xall, 0, i, mp, right, nsem.at[i, 0])
        pass_on(call, 1, i, mp, left, nsem.at[i, 0])
        pass_on(call, 1, i, mp, right, nsem.at[i, 1])
        pass_on(xall, 0, i, mp, left, nsem.at[i, 1])

    def pair(i):
        return xall.at[i, pl.ds(0, 2 * feats), :]

    for i in range(AHEAD):
        start_own(i)
    fetched(call.at[0, pl.ds(0, (NC - AHEAD) * feats), :], lsem.at[6])
    fetched(xall.at[0, pl.ds(0, (NC - AHEAD) * feats), :], lsem.at[7])
    for i in range(AHEAD, NC):
        mask_cot(i)
    for i in range(NC):
        pass_on(xall, 0, i, mp, mate, msem.at[i])
        pass_on(call, 1, i, mp, mate, msem.at[i])
    lane8 = lax.broadcasted_iota(jnp.int32, (8, 128), 1)
    mine = jnp.zeros((8, 128), jnp.int32)
    for b in range(blocks):
        mine = jnp.where(lane8 == b, ranks[b], mine)
    ers[...] = mine
    erb[dp] = mine
    for t in range(1, N_DP):
        send(ers, erb.at[dp], xs.at[0], xr.at[0], dp_at(t), mp).start()

    for k, (src, dst) in enumerate(weights):
        fetched(dst, lsem.at[2 + k])
    for j in range(wus.shape[1] // 128):
        wut[j * 128 : (j + 1) * 128, :] = wus[:, j * 128 : (j + 1) * 128].T
    for j in range(wds.shape[1] // 128):
        wdt[j * 128 : (j + 1) * 128, :] = wds[:, j * 128 : (j + 1) * 128].T
    quh[...] = stack2(qus[...])
    qdh[...] = stack2(qds[...])
    for ph in range(2):
        proj[ph] = jnp.zeros_like(proj[ph])
        small[ph] = jnp.zeros_like(small[ph])

    def start_out(i):
        send(outp.at[i, 1 - c], po.at[i], ossem.at[0], osem.at[i], dp, mate).start()

    def out_sum(i):
        arrived(po.at[i], osem.at[i])
        osb[i] = (outp[i, c].astype(F32) + po[i].astype(F32)).astype(BF16)

    def work_a(i):
        pre = mm(wut[...], xall[i])
        grad = mm(wds[...], call[i])
        sig = jax.nn.sigmoid(1.702 * pre)
        act = pre * sig
        hid[i] = act.astype(BF16)
        gp[i] = (grad * (sig + 1.702 * act * (1.0 - sig))).astype(BF16)

    def work_b(i):
        o = mm(wdt[...], hid[i]).astype(BF16)
        for m in range(N_MP):
            at = (m // 2) * feats
            outp[i, m % 2, at : at + feats, :] = o[m * feats : (m + 1) * feats]
        start_out(i)

    def big_add(ph, rows64, other):
        big = fold2(mm_nt(stack2(rows64), other))
        proj[ph, 0] += big[:, :half]
        proj[ph, 1] += big[:, half:]

    def small_add(ph, rows64, other):
        small[ph] += fold2(mm_nt(stack2(rows64), other))

    def add_projection(i):
        big_add(0, fold2(mm(quh[...], gp[i])), xall[i])
        small_add(0, fold2(mm(qdh[...], call[i])), hid[i])

    def piece(first, owner):
        at = pl.multiple_of((owner // 2) * feats, 32)
        return osb.at[pl.ds(first, HALF), pl.ds(at, feats), :]

    def own_rows(i, owner):
        return osb[i, pl.ds(pl.multiple_of((owner // 2) * feats, 32), feats), :]

    def send_a(j):
        y_send(osb.at[j, pl.ds(pl.multiple_of((right // 2) * feats, 32), feats), :], da.at[j], 4, right)

    def send_b(i):
        j = i - HALF
        y_send(osb.at[i, pl.ds(pl.multiple_of((far // 2) * feats, 32), feats), :], rb.at[j], 1, right)
        y_send(osb.at[i, pl.ds(pl.multiple_of((left // 2) * feats, 32), feats), :], db.at[j], 5, left)

    def y_send(src, dst, group, to):
        send(src, dst, yssem.at[group], ysem.at[group], dp, to).start()

    def mate_start(ph):
        send(proj.at[ph, 1 - c], pbuf.at[ph], mrs.at[ph, 0], mrr.at[ph, 0], dp, mate).start()

    def mate_end(ph):
        arrived(pbuf.at[ph], mrr.at[ph, 0])
        return proj[ph, c] + pbuf[ph]

    def scatter(q, value):
        for j in range(N_DP):
            rsb[q, j] = value[4 * j : 4 * j + 4]
        for t in range(1, N_DP):
            to = dp_at(t)
            send(rsb.at[q, to], rcv.at[q, dp], ars.at[q, 0], arr.at[q, 0], to, mp).start()
        rcv[q, dp] = rsb[q, dp]

    def collect(q):
        arrived(rcv.at[q, pl.ds(0, N_DP - 1)], arr.at[q, 0])
        total = rcv[q, 0]
        for j in range(1, N_DP):
            total = total + rcv[q, j]
        return total

    def y_start(ph, q, total):
        ysend[ph] = total
        for t in range(1, N_Y):
            to = ((y + t) % N_Y) * 2 + c
            send(ysend.at[ph], ybuf.at[ph, y], ars.at[q, 2], arr.at[q, 2], dp, to).start()
        ybuf[ph, y] = total

    def y_end(ph, q):
        arrived(ybuf.at[ph, pl.ds(0, N_Y - 1)], arr.at[q, 2])
        total = ybuf[ph, 0]
        for j in range(1, N_Y):
            total = total + ybuf[ph, j]
        return total

    def spread(q, total):
        agb[q, dp] = total
        for t in range(1, N_DP):
            send(agb.at[q, dp], agb.at[q, dp], ars.at[q, 1], arr.at[q, 1], dp_at(t), mp).start()

    def small_end(ph, q):
        arrived(agb.at[q, pl.ds(0, N_DP - 1)], arr.at[q, 1])
        for j in range(N_DP):
            small[ph, 4 * j : 4 * j + 4] = agb[q, j]
        return small[ph]

    def big_start(ph, q):
        arrived(agb.at[q, pl.ds(0, N_DP - 1)], arr.at[q, 1])
        for j in range(N_DP):
            bigf[ph, c, 4 * j : 4 * j + 4] = agb[q, j]
        send(bigf.at[ph, c], bigf.at[ph, c], mrs.at[ph, 1], mrr.at[ph, 1], dp, mate).start()

    def big_end(ph):
        arrived(bigf.at[ph, 0], mrr.at[ph, 1])
        return jnp.concatenate([bigf[ph, 0], bigf[ph, 1]], axis=1)

    def step(i, carry):
        @pl.when(i < NC)
        def _():
            arrived(pair(i), nsem.at[i, 0])
            pass_on(xall, 0, i, left, right, nsem.at[i, 2])
            pass_on(call, 1, i, right, left, nsem.at[i, 2])

            @pl.when(i + AHEAD < NC)
            def _():
                start_own(i + AHEAD)

            pass_on(xall, 0, i, left, mate, msem.at[i])
            pass_on(call, 1, i, right, mate, msem.at[i])

        @pl.when(jnp.logical_and(i > 1, i < NC + 2))
        def _():
            arrived(xall.at[i - 2], msem.at[i - 2])
            work_a(i - 2)

        @pl.when(i < NC)
        def _():
            arrived(pair(i), nsem.at[i, 1])
            pass_on(call, 1, i, left, mate, msem.at[i])
            pass_on(xall, 0, i, right, mate, msem.at[i])

        @pl.when(jnp.logical_and(i > 1, i < NC + 2))
        def _():
            add_projection(i - 2)

        @pl.when(jnp.logical_and(i > 2, i <= NC))
        def _():
            out_sum(i - 3)

        @pl.when(i == NC)
        def _():
            y_send(piece(0, far), ra, 0, left)
            send_b(HALF)
            for j in range(HALF - 1):
                send_a(j)

        @pl.when(jnp.logical_and(i > 0, i <= NC))
        def _():
            arrived(pair(i - 1), nsem.at[i - 1, 2])
            pass_on(xall, 0, i - 1, far, mate, msem.at[i - 1])
            pass_on(call, 1, i - 1, far, mate, msem.at[i - 1])

        @pl.when(i == NC + 3)
        def _():
            scatter(0, mate_end(0))

        @pl.when(jnp.logical_or(jnp.logical_and(i > 1, i < NC), i > NC + 1))
        def _():
            work_b(jnp.where(i < NC, i - 2, i - 4))

        @pl.when(i == NC + 1)
        def _():
            mate_start(0)
            scatter(1, small[0])

        return carry

    lax.fori_loop(0, NC + 4, step, 0)

    def start_slots(k, group):
        for t in GROUPS[group]:
            to = dp_at(t)
            send(a2s.at[k, to], a2o.at[k, dp], a2ss.at[k], a2rr.at[k], to, mp).start()

    def out_landed(k):
        arrived(a2o.at[k, pl.ds(0, N_DP - 1)], a2rr.at[k])

    for i in range(HALF + 1, NC):
        out_sum(i)
        send_b(i)
    send_a(HALF - 1)
    arrived(ra, ysem.at[0])
    for i in range(HALF):
        fa[i] = (own_rows(i, left).astype(F32) + ra[i].astype(F32)).astype(BF16)
    spread(1, collect(1))
    y_start(0, 0, collect(0))
    y_send(fa, ea, 2, left)
    arrived(rb, ysem.at[1])
    for i in range(HALF):
        fb[i] = (own_rows(HALF + i, right).astype(F32) + rb[i].astype(F32)).astype(BF16)
    y_send(fb, eb, 3, right)
    spread(0, y_end(0, 0))
    proj_down = small_end(0, 1)
    quh[:, :half] = stack2(proj_down)

    def fresh_down(i, carry):
        big_add(1, fold2(mm(quh[...], hid[i])), call[i])
        return carry

    lax.fori_loop(0, NC, fresh_down, 0, unroll=2)
    mate_start(1)
    gram_d = gram_of(proj_down)
    gbuf[mp] = jnp.concatenate([gram_d[: RANK // 2], gram_d[RANK // 2 :]], axis=1)
    for t in range(1, N_MP):
        send(gbuf.at[mp], gbuf.at[mp], xs.at[1], xr.at[1], dp, mp_at(t)).start()
    big_start(0, 0)
    scatter(2, mate_end(1))
    arrived(ea, ysem.at[2])
    arrived(eb, ysem.at[3])
    arrived(da, ysem.at[4])
    arrived(db, ysem.at[5])
    for b in range(blocks):
        i, at = b // per, (b % per) * BLOCK
        direct, summed = (da, ea) if i < HALF else (db, eb)
        lanes = slice(at, at + BLOCK)
        total = own_rows(i, mp)[:, lanes].astype(F32)
        total = total + direct[i % HALF, :, lanes].astype(F32) + summed[i % HALF, :, lanes].astype(F32)
        ob[b] = jnp.where(token < fills[b], total, 0.0).astype(BF16)
    for j in range(N_DP):
        first = jnp.int32(0)
        second = jnp.int32(0)
        for b in range(blocks - 1, -1, -1):
            here = ranks[b] == j
            second = jnp.where(here, first, second)
            first = jnp.where(here, b, first)
        a2s[0, j] = ob[first]
        a2s[1, j] = ob[second]
    start_slots(0, 0)
    start_slots(0, 1)
    for k in range(CAP):
        pltpu.make_async_copy(a2s.at[k, dp], a2o.at[k, dp], lsem.at[k]).start()
    proj_up = big_end(0)
    qdh[...] = stack2(proj_up)

    def fresh_up(i, carry):
        small_add(1, fold2(mm(qdh[...], xall[i])), gp[i])
        return carry


    lax.fori_loop(0, NC, fresh_up, 0, unroll=2)
    scatter(3, small[1])
    start_slots(0, 2)
    start_slots(0, 3)
    y_start(1, 2, collect(2))
    elim[0] = identity_at_right((RANK, 2 * RANK))
    elim[0, :, :RANK] = gram_of(proj_up)
    arrived(gbuf.at[pl.ds(0, N_MP - 1)], xr.at[1])
    gram_d = gbuf[0]
    for j in range(1, N_MP):
        gram_d = gram_d + gbuf[j]
    elim[1] = identity_at_right((RANK, 2 * RANK))
    elim[1, : RANK // 2, :RANK] = gram_d[:, :RANK]
    elim[1, RANK // 2 :, :RANK] = gram_d[:, RANK:]
    start_slots(1, 0)
    elim[...] = eliminate(elim[...], 0, 8)
    spread(2, y_end(1, 2))
    start_slots(1, 1)
    elim[...] = eliminate(elim[...], 8, 24)
    spread(3, collect(3))
    start_slots(1, 2)
    start_slots(1, 3)
    elim[...] = eliminate(elim[...], 24, RANK - 1)
    inv_u = left4(inverse_of_factor(elim[0]).T)
    inv_d = left4(inverse_of_factor(elim[1]).T)
    f4u[...] = left4(mm_tn(inv_u, right4(proj_up))).T
    f4d[...] = left4(mm_tn(inv_d, right4(proj_down))).T
    pltpu.make_async_copy(f4u, a4u, lsem.at[2]).start()
    pltpu.make_async_copy(f4d, a4d, lsem.at[3]).start()
    arrived(erb.at[pl.ds(0, N_DP - 1)], xr.at[0])
    for r in range(N_DP):
        ef[r : r + 1, :] = erb[r, 0:1, :]
    pltpu.make_async_copy(ef, era_out, lsem.at[4]).start()
    big_start(1, 2)
    out_landed(0)
    new_u = mm_tn(inv_u, right4(small_end(1, 3)))
    fu[...] = new_u
    pltpu.make_async_copy(fu, qnu, lsem.at[5]).start()
    new_d = mm_tn(inv_d, right4(big_end(1)))
    fd[...] = new_d
    pltpu.make_async_copy(fd, qnd, lsem.at[6]).start()
    out_landed(1)

    pltpu.make_async_copy(f4u, a4u, lsem.at[2]).wait()
    pltpu.make_async_copy(f4d, a4d, lsem.at[3]).wait()
    pltpu.make_async_copy(ef, era_out, lsem.at[4]).wait()
    pltpu.make_async_copy(fu, qnu, lsem.at[5]).wait()
    pltpu.make_async_copy(fd, qnd, lsem.at[6]).wait()
    left_here(xall.at[:, pl.ds(0, 7 * feats), :], gsem.at[0])
    left_here(call.at[:, pl.ds(0, 7 * feats), :], gsem.at[1])
    left_here(po, ossem.at[0])
    left_here(erb.at[pl.ds(0, N_DP - 1)], xs.at[0])
    left_here(gbuf.at[pl.ds(0, N_MP - 1)], xs.at[1])
    for group, ref in enumerate((ra, rb, ea, eb, da, db)):
        left_here(ref, yssem.at[group])
    for ph in range(2):
        left_here(pbuf.at[ph], mrs.at[ph, 0])
        left_here(bigf.at[ph, 0], mrs.at[ph, 1])
        left_here(ybuf.at[ph, pl.ds(0, N_Y - 1)], ars.at[2 * ph, 2])
    for q in range(4):
        left_here(rcv.at[q, pl.ds(0, N_DP - 1)], ars.at[q, 0])
        left_here(agb.at[q, pl.ds(0, N_DP - 1)], ars.at[q, 1])
    for k in range(CAP):
        left_here(a2s.at[k, pl.ds(0, N_DP - 1)], a2ss.at[k])
        pltpu.make_async_copy(a2s.at[k, dp], a2o.at[k, dp], lsem.at[k]).wait()


def layer_kernel(ranks, fills, pt, ct, wu, wd, qu, qd):
    feats, tokens = pt.shape
    tc = tokens // NC
    width, ff = wu.shape
    half = width // 2
    sm = pl.BlockSpec(memory_space=pltpu.SMEM)
    anywhere = pl.BlockSpec(memory_space=pl.ANY)
    shape = jax.ShapeDtypeStruct
    outs = [
        shape((CAP, N_DP, feats, BLOCK), BF16),
        shape((width, 4 * RANK), BF16),
        shape((ff, 4 * RANK), BF16),
        shape((N_DP, 128), jnp.int32),
        shape((RANK, ff), F32),
        shape((RANK, width), F32),
    ]
    dma = pltpu.SemaphoreType.DMA
    scratch = [
        pltpu.VMEM((NC, width, tc), BF16),
        pltpu.VMEM((NC, width, tc), BF16),
        pltpu.VMEM((NC, ff, tc), BF16),
        pltpu.VMEM((NC, ff, tc), BF16),
        pltpu.VMEM((width, ff), BF16),
        pltpu.VMEM((ff, width), BF16),
        pltpu.VMEM((RANK, ff), F32),
        pltpu.VMEM((RANK, width), F32),
        pltpu.VMEM((ff, width), BF16),
        pltpu.VMEM((width, ff), BF16),
        pltpu.VMEM((2 * RANK, ff), BF16),
        pltpu.VMEM((2 * RANK, width), BF16),
        pltpu.VMEM((2, 2, RANK, half), F32),
        pltpu.VMEM((2, RANK, ff), F32),
        pltpu.VMEM((2, RANK, half), F32),
        pltpu.VMEM((4, N_DP, 4, half), F32),
        pltpu.VMEM((4, N_DP, 4, half), F32),
        pltpu.VMEM((2, 4, half), F32),
        pltpu.VMEM((2, N_Y, 4, half), F32),
        pltpu.VMEM((4, N_DP, 4, half), F32),
        pltpu.VMEM((2, 2, RANK, half), F32),
        pltpu.VMEM((2, RANK, 2 * RANK), F32),
        pltpu.VMEM((N_MP, RANK // 2, 2 * RANK), F32),
        pltpu.VMEM((NC, 2, N_Y * feats, tc), BF16),
        pltpu.VMEM((NC, N_Y * feats, tc), BF16),
        pltpu.VMEM((NC, N_Y * feats, tc), BF16),
    ]
    scratch += [pltpu.VMEM((HALF, feats, tc), BF16) for _ in range(8)]
    scratch += [
        pltpu.VMEM((tokens // BLOCK, feats, BLOCK), BF16),
        pltpu.VMEM((CAP, N_DP, feats, BLOCK), BF16),
        pltpu.VMEM((width, 4 * RANK), BF16),
        pltpu.VMEM((ff, 4 * RANK), BF16),
        pltpu.VMEM((RANK, ff), F32),
        pltpu.VMEM((RANK, width), F32),
        pltpu.VMEM((N_DP, 128), jnp.int32),
        pltpu.VMEM((8, 128), jnp.int32),
        pltpu.VMEM((N_DP, 8, 128), jnp.int32),
        dma((8,)),
        dma((NC, 3)),
        dma((NC,)),
        dma((2,)),
        dma((NC,)),
        dma((1,)),
        dma((6,)),
        dma((6,)),
        dma((4, 3)),
        dma((4, 3)),
        dma((2, 2)),
        dma((2, 2)),
        dma((2,)),
        dma((2,)),
        dma((CAP,)),
        dma((CAP,)),
    ]
    return pl.pallas_call(
        kernel_body,
        out_shape=outs,
        in_specs=[sm] * 2 + [anywhere] * 6,
        out_specs=[anywhere] * len(outs),
        scratch_shapes=scratch,
        compiler_params=pltpu.CompilerParams(
            collective_id=0, has_side_effects=True, vmem_limit_bytes=60 * 1024 * 1024
        ),
        name="layer",
    )(ranks, fills, pt, ct, wu, wd, qu, qd)


def finish_body(
    ranks, landed, a4u, a4d, qnu, qnd,
    enc, up, down, new_u, new_d,
    blocks, placed, ups, downs, b4u, b4d, origin, sems,
):
    me = lax.axis_index("dp")
    for k in range(CAP):
        pltpu.make_async_copy(landed.at[k], blocks.at[pl.ds(k * N_DP, N_DP)], sems.at[10 + k]).start()
    copies = []
    for k, (src, dst) in enumerate(((qnu, new_u), (qnd, new_d))):
        copy = pltpu.make_async_copy(src, dst, sems.at[13 + k])
        copy.start()
        copies.append(copy)
    b4u[...] = right4(qnu[...])
    b4d[...] = right4(qnd[...])
    for k, (a, b, stage, out) in enumerate(((a4u, b4u, ups, up), (a4d, b4d, downs, down))):
        pieces = 2
        size = stage.shape[0] // pieces
        for j in range(pieces):
            at = pl.ds(j * size, size)
            stage[at, :] = mm(a[at, :], b[...])
            copy = pltpu.make_async_copy(stage.at[at, :], out.at[at, :], sems.at[k * pieces + j])
            copy.start()
            copies.append(copy)
    for slot in range(RMAX + 1):
        origin[slot] = CAP * N_DP
    filled = jnp.int32(0)
    for r in range(N_DP):
        seen = jnp.int32(0)
        for b in range(BLK_DEV):
            hit = (ranks[r, b] == me).astype(jnp.int32)
            held = origin[filled]
            origin[filled] = jnp.where(hit > 0, seen * N_DP + r, held)
            seen = seen + hit
            filled = filled + hit
    blocks[CAP * N_DP] = jnp.zeros_like(blocks[CAP * N_DP])
    for k in range(CAP):
        pltpu.make_async_copy(landed.at[k], blocks.at[pl.ds(k * N_DP, N_DP)], sems.at[10 + k]).wait()
    for slot in range(RMAX):
        placed[:, slot * BLOCK : (slot + 1) * BLOCK] = blocks[origin[slot]]
    copy = pltpu.make_async_copy(placed, enc, sems.at[12])
    copy.start()
    copies.append(copy)
    for copy in copies:
        copy.wait()


def finish(landed, a4u, a4d, ranks, qnu, qnd):
    feats = landed.shape[2]
    width, ff = a4u.shape[0], a4d.shape[0]
    vm = pl.BlockSpec(memory_space=pltpu.VMEM)
    anywhere = pl.BlockSpec(memory_space=pl.ANY)
    shape = jax.ShapeDtypeStruct
    return pl.pallas_call(
        finish_body,
        out_shape=[
            shape((feats, RMAX * BLOCK), BF16),
            shape((width, ff), F32),
            shape((ff, width), F32),
            shape(qnu.shape, F32),
            shape(qnd.shape, F32),
        ],
        in_specs=[pl.BlockSpec(memory_space=pltpu.SMEM), anywhere] + [vm] * 4,
        out_specs=[anywhere] * 5,
        scratch_shapes=[
            pltpu.VMEM((CAP * N_DP + 1, *landed.shape[2:]), BF16),
            pltpu.VMEM((feats, RMAX * BLOCK), BF16),
            pltpu.VMEM((width, ff), F32),
            pltpu.VMEM((ff, width), F32),
            pltpu.VMEM((4 * RANK, ff), BF16),
            pltpu.VMEM((4 * RANK, width), BF16),
            pltpu.SMEM((RMAX + 1,), jnp.int32),
            pltpu.SemaphoreType.DMA((15,)),
        ],
        name="finish",
    )(ranks, landed, a4u, a4d, qnu, qnd)


def local(patches, cotangent, encoder_rank, block_fill, w_up, w_down, q_up, q_down):
    results = layer_kernel(
        encoder_rank, block_fill, patches.T, cotangent.T, w_up, w_down, q_up.T, q_down.T
    )
    encoded, approx_up, approx_down, new_u, new_d = finish(*results)
    return (encoded.T, approx_up, approx_down, new_u.T, new_d.T)


def solution(mesh):
    in_specs = (
        P("dp", "mp"), P("dp", "mp"), P("dp"), P("dp"), P(None, "mp"), P("mp", None), P("mp", None), P(),
    )
    out_specs = (P("dp", "mp"), P(None, "mp"), P("mp", None), P("mp", None), P())
    return jax.shard_map(local, mesh=mesh, in_specs=in_specs, out_specs=out_specs, check_vma=False)
```
